32 devices in a mesh: data: 2 (over x), node: 4 (over z), expert: 4 (over y, core).
Axes of the slice: x: 2, y: 2, z: 4, core: 2. Of those that a mesh axis runs over, the one named last changes fastest.
Arguments:
- tokens: bfloat16 [32768, 768], P(('data', 'node', 'expert')), parts along dimension 0
- expert_ids: int32 [32768, 1], P(('data', 'node', 'expert')), parts along dimension 0
- gate_weights: float32 [32768, 1], P(('data', 'node', 'expert')), parts along dimension 0
- slot_ids: int32 [32768, 1], P(('data', 'node', 'expert')), parts along dimension 0
- w_gate: bfloat16 [16, 768, 3072], P(('node', 'expert'))
- w_up: bfloat16 [16, 768, 3072], P(('node', 'expert'))
- w_down: bfloat16 [16, 3072, 768], P(('node', 'expert'))
Outputs:
- output: bfloat16 [32768, 768], P(('data', 'node', 'expert')), parts along dimension 0
There are 2 independent parts. The reference program is written for one: setup_inputs(seed, part) draws one part's arguments, and reference() takes and returns one part's arrays. A program takes and returns all parts, laid end to end along the dimension named above; an argument that names none is the same for every part.
All inputs are finite; a program needn't handle non-finite values.
Results may differ from the reference program's by a relative error of at most 0.001.
Values are sent between devices in bfloat16 or wider.
A program may use at most 1 GiB of HBM per device.

```python
import jax
import jax.numpy as jnp
from jax import lax

EXPERTS = 16
D = 768
FF = 3072
TOP = 1
TOKENS_DEV = 1024
GROUP = 16
CAP = 128

TOKENS = GROUP * TOKENS_DEV


def device_slots(flat_ids):
    choice_count = flat_ids.shape[0]
    sort_order = jnp.argsort(flat_ids, stable=True)
    sorted_ids = flat_ids[sort_order]
    counts = jnp.zeros((EXPERTS,), jnp.int32).at[flat_ids].add(1)
    starts = jnp.cumsum(counts) - counts
    rank_sorted = jnp.arange(choice_count, dtype=jnp.int32) - starts[sorted_ids]
    rank_all = jnp.zeros((choice_count,), jnp.int32).at[sort_order].set(rank_sorted)
    return jnp.where(rank_all < CAP, rank_all, -1)


def draw_routing(key):
    sub_keys = jax.random.split(key, 5)
    hot_first = jax.random.randint(sub_keys[0], (), 0, EXPERTS)
    pick_hot = jax.random.randint(sub_keys[1], (TOKENS,), 0, 4)
    hot_base = jax.random.randint(sub_keys[2], (TOKENS,), 0, max(EXPERTS // 4, 1))
    any_base = jax.random.randint(sub_keys[3], (TOKENS,), 0, EXPERTS)
    base_ids = jnp.where(pick_hot == 0, hot_base, any_base)
    local_row = jnp.arange(TOKENS, dtype=jnp.int32) % TOKENS_DEV
    base_ids = jnp.where(local_row < CAP, 0, base_ids)
    step_max = (EXPERTS - 1) // max(TOP - 1, 1)
    step_sizes = jax.random.randint(sub_keys[4], (TOKENS, TOP), 1, step_max + 1)
    step_sizes = step_sizes.at[:, 0].set(0)
    offsets = jnp.cumsum(step_sizes, axis=1)
    expert_ids = ((base_ids[:, None] + hot_first + offsets) % EXPERTS).astype(jnp.int32)
    slot_ids = jax.vmap(device_slots)(expert_ids.reshape(GROUP, TOKENS_DEV * TOP))
    return expert_ids, slot_ids.reshape(TOKENS, TOP).astype(jnp.int32)


def setup_inputs(seed: int = 0, part: int = 0) -> dict:
    part_key = jax.random.fold_in(jax.random.key(seed), part)
    key_tokens, key_route, key_gates = jax.random.split(part_key, 3)
    key_gate_w, key_up_w, key_down_w = jax.random.split(jax.random.key(seed + 1), 3)
    tokens = jax.random.normal(key_tokens, (TOKENS, D), jnp.float32).astype(jnp.bfloat16)
    expert_ids, slot_ids = draw_routing(key_route)
    gate_weights = (0.5 + jax.random.uniform(key_gates, (TOKENS, TOP), jnp.float32)) * TOP ** -0.5
    w_gate = (jax.random.normal(key_gate_w, (EXPERTS, D, FF), jnp.float32) * D ** -0.5).astype(jnp.bfloat16)
    w_up = (jax.random.normal(key_up_w, (EXPERTS, D, FF), jnp.float32) * D ** -0.5).astype(jnp.bfloat16)
    w_down = (jax.random.normal(key_down_w, (EXPERTS, FF, D), jnp.float32) * FF ** -0.5).astype(jnp.bfloat16)
    return {"tokens": tokens, "expert_ids": expert_ids, "gate_weights": gate_weights, "slot_ids": slot_ids, "w_gate": w_gate, "w_up": w_up, "w_down": w_down}


def expert_block(expert_rows, gate_mat, up_mat, down_mat):
    proj_gate = jnp.dot(expert_rows, gate_mat, preferred_element_type=jnp.float32)
    proj_up = jnp.dot(expert_rows, up_mat, preferred_element_type=jnp.float32)
    hidden = (jax.nn.silu(proj_gate) * proj_up).astype(jnp.bfloat16)
    return jnp.dot(hidden, down_mat, preferred_element_type=jnp.float32).astype(jnp.bfloat16)


def reference(tokens, expert_ids, gate_weights, slot_ids, w_gate, w_up, w_down):
    buffer_rows = GROUP * CAP
    source_dev = (jnp.arange(TOKENS, dtype=jnp.int32) // TOKENS_DEV)[:, None]
    kept = slot_ids >= 0
    flat_pos = jnp.where(kept, expert_ids * buffer_rows + source_dev * CAP + slot_ids, EXPERTS * buffer_rows).reshape(-1)
    tok_index = jnp.broadcast_to(jnp.arange(TOKENS, dtype=jnp.int32)[:, None], (TOKENS, TOP)).reshape(-1)
    src_table = jnp.full((EXPERTS * buffer_rows,), TOKENS, jnp.int32).at[flat_pos].set(tok_index, mode="drop")
    gate_table = jnp.zeros((EXPERTS * buffer_rows,), jnp.float32).at[flat_pos].set(gate_weights.reshape(-1), mode="drop")

    def one_expert(out_sum, operands):
        src_rows, row_gates, gate_mat, up_mat, down_mat = operands
        expert_rows = jnp.take(tokens, src_rows, axis=0, mode="fill", fill_value=0)
        expert_out = expert_block(expert_rows, gate_mat, up_mat, down_mat)
        out_sum = out_sum.at[src_rows].add(row_gates[:, None] * expert_out.astype(jnp.float32), mode="drop")
        return out_sum, None

    out_sum, _ = lax.scan(one_expert, jnp.zeros((TOKENS, D), jnp.float32), (src_table.reshape(EXPERTS, buffer_rows), gate_table.reshape(EXPERTS, buffer_rows), w_gate, w_up, w_down))
    return out_sum.astype(jnp.bfloat16)
```

```python
import functools

import jax
import jax.numpy as jnp
from jax import lax
from jax.experimental import pallas as pl
from jax.experimental.pallas import tpu as pltpu
from jax.sharding import PartitionSpec as P

CAP_FACTOR = 2
MESH = pl.DeviceIdType.MESH
FF_TILE = 512
REMOTE = 12


def capacity(rows, top_k, experts):
    return ((CAP_FACTOR * rows * top_k + 8 * experts - 1) // (8 * experts)) * 8


def flip(value, by):
    return 2 * ((value // 2 + by // 2) % 2) + (value + by) % 2


def partner(step):
    node, expert = lax.axis_index("node"), lax.axis_index("expert")
    far = 1 - step // REMOTE
    by_node = far * (1 + (step % 3 + 1) % 3)
    by_expert = far * (step // 3) + (1 - far) * (step - REMOTE)
    return flip(node, by_node), flip(expert, by_expert)


def layer_kernel(slot_count, tok_ref, pos_row_ref, pos_col_ref, gate_hbm, up_hbm, down_hbm, out_ref,
                 gate_w, up_w, down_w, send, recv, result, back, hidden, total,
                 w_sem, go_sem, come_sem, ret_go_sem, ret_come_sem):
    rows, width = tok_ref.shape
    steps = 16
    loads = [pltpu.make_async_copy(src.at[0], dst, w_sem.at[i]) for i, (src, dst) in enumerate(
        ((gate_hbm, gate_w), (up_hbm, up_w), (down_hbm, down_w)))]
    for load in loads:
        load.start()

    barrier = pltpu.get_barrier_semaphore()

    def greet(step, carry):
        node, expert = partner(step)
        pl.semaphore_signal(barrier, inc=1, device_id={"node": node, "expert": expert}, device_id_type=MESH)
        return carry

    lax.fori_loop(0, REMOTE, greet, 0)
    lax.fori_loop(REMOTE + 1, steps, greet, 0)

    def dispatch_copy(step):
        node, expert = partner(step)
        return pltpu.make_async_remote_copy(
            src_ref=send.at[step], dst_ref=recv.at[step], send_sem=go_sem.at[step], recv_sem=come_sem.at[step],
            device_id={"node": node, "expert": expert}, device_id_type=MESH)

    def return_copy(step):
        node, expert = partner(step)
        return pltpu.make_async_remote_copy(
            src_ref=result.at[step], dst_ref=back.at[step], send_sem=ret_go_sem.at[step], recv_sem=ret_come_sem.at[step],
            device_id={"node": node, "expert": expert}, device_id_type=MESH)

    def pick(step):
        node, expert = partner(step)
        first = (node * 4 + expert) * slot_count
        slot = lax.broadcasted_iota(jnp.int32, (slot_count, rows), 0) + first
        chosen = (pos_row_ref[...] == slot).astype(jnp.float32).astype(jnp.bfloat16)
        return jnp.dot(chosen, tok_ref[...], preferred_element_type=jnp.float32).astype(jnp.bfloat16)

    send[0] = pick(0)
    pl.semaphore_wait(barrier, steps - 1)
    dispatch_copy(0).start()

    def dispatch(step, carry):
        send[step] = pick(step)
        dispatch_copy(step).start()
        return carry

    lax.fori_loop(1, REMOTE, dispatch, 0)
    lax.fori_loop(REMOTE + 1, steps, dispatch, 0)
    recv[REMOTE] = pick(REMOTE)
    for load in loads:
        load.wait()

    def ffn(step, dst):
        block = recv[step]
        ff = hidden.shape[1]
        for start in range(0, ff, FF_TILE):
            cols = slice(start, start + FF_TILE)
            gate = jnp.dot(block, gate_w[:, cols], preferred_element_type=jnp.float32)
            up = jnp.dot(block, up_w[:, cols], preferred_element_type=jnp.float32)
            hidden[:, cols] = (jax.nn.silu(gate) * up).astype(jnp.bfloat16)
        dst[step] = jnp.dot(hidden[...], down_w[...], preferred_element_type=jnp.float32).astype(jnp.bfloat16)

    def compute(order, carry):
        step = (order + REMOTE) % steps

        @pl.when(step != REMOTE)
        def _():
            dispatch_copy(step).wait_recv()

        ffn(step, result)

        @pl.when(step != REMOTE)
        def _():
            return_copy(step).start()

        return carry

    lax.fori_loop(0, steps, compute, 0)
    back[REMOTE] = result[REMOTE]

    group = 4
    total[...] = jnp.zeros_like(total)

    def combine(order, carry):
        base = ((order + REMOTE // group) % (steps // group)) * group
        picks = []
        for i in range(group):
            step = base + i

            @pl.when(step != REMOTE)
            def _():
                return_copy(step).wait_recv()

            node, expert = partner(step)
            first = (node * 4 + expert) * slot_count
            slot = lax.broadcasted_iota(jnp.int32, (rows, slot_count), 1) + first
            picks.append((pos_col_ref[...] == slot).astype(jnp.float32).astype(jnp.bfloat16))
        chosen = jnp.concatenate(picks, axis=1)
        rets = back[pl.ds(base, group)].reshape(group * slot_count, width)
        total[...] += jnp.dot(chosen, rets, preferred_element_type=jnp.float32)
        return carry

    lax.fori_loop(0, steps // group, combine, 0)
    out_ref[...] = total[...].astype(out_ref.dtype)

    def drain(step, carry):
        dispatch_copy(step).wait_send()
        return_copy(step).wait_send()
        return carry

    lax.fori_loop(0, REMOTE, drain, 0)
    lax.fori_loop(REMOTE + 1, steps, drain, 0)


def solution(mesh):
    group_size = mesh.shape["node"] * mesh.shape["expert"]
    tok_spec = P(("data", "node", "expert"), None)
    weight_spec = P(("node", "expert"), None, None)

    def local_layer(tokens, expert_ids, gate_weights, slot_ids, w_gate, w_up, w_down):
        rows, width = tokens.shape
        ff = w_gate.shape[2]
        slot_count = capacity(rows, 1, group_size)
        flat_pos = jnp.where(slot_ids >= 0, expert_ids * slot_count + slot_ids, group_size * slot_count)
        vmem = pl.BlockSpec(memory_space=pltpu.VMEM)
        hbm = pl.BlockSpec(memory_space=pl.ANY)
        block = (group_size, slot_count, width)
        picked = pl.pallas_call(
            functools.partial(layer_kernel, slot_count),
            out_shape=jax.ShapeDtypeStruct((rows, width), jnp.bfloat16),
            in_specs=[vmem] * 3 + [hbm] * 3,
            out_specs=vmem,
            scratch_shapes=[
                pltpu.VMEM((width, ff), jnp.bfloat16),
                pltpu.VMEM((width, ff), jnp.bfloat16),
                pltpu.VMEM((ff, width), jnp.bfloat16),
                pltpu.VMEM(block, jnp.bfloat16),
                pltpu.VMEM(block, jnp.bfloat16),
                pltpu.VMEM(block, jnp.bfloat16),
                pltpu.VMEM(block, jnp.bfloat16),
                pltpu.VMEM((slot_count, ff), jnp.bfloat16),
                pltpu.VMEM((rows, width), jnp.float32),
                pltpu.SemaphoreType.DMA((3,)),
                pltpu.SemaphoreType.DMA((group_size,)),
                pltpu.SemaphoreType.DMA((group_size,)),
                pltpu.SemaphoreType.DMA((group_size,)),
                pltpu.SemaphoreType.DMA((group_size,)),
            ],
            compiler_params=pltpu.CompilerParams(
                collective_id=0, has_side_effects=True, vmem_limit_bytes=60 * 1024 * 1024),
            name="moe_layer",
        )(tokens, flat_pos.reshape(1, rows), flat_pos, w_gate, w_up, w_down)
        return (gate_weights * picked.astype(jnp.float32)).astype(jnp.bfloat16)

    return jax.shard_map(local_layer, mesh=mesh, in_specs=(tok_spec,) * 4 + (weight_spec,) * 3,
                         out_specs=tok_spec, check_vma=False)
```

```python
import functools

import jax
import jax.numpy as jnp
from jax import lax
from jax.experimental import pallas as pl
from jax.experimental.pallas import tpu as pltpu
from jax.sharding import PartitionSpec as P

CAP_FACTOR = 2
MESH = pl.DeviceIdType.MESH
FF_TILE = 512
REMOTE = 12
BASE = 64
SPILL = 224
LIST = SPILL + 16
PADDED = 256


def capacity(rows, top_k, experts):
    return ((CAP_FACTOR * rows * top_k + 8 * experts - 1) // (8 * experts)) * 8


def flip(value, by):
    return 2 * ((value // 2 + by // 2) % 2) + (value + by) % 2


def place(by_node, by_expert):
    return {"node": flip(lax.axis_index("node"), by_node), "expert": flip(lax.axis_index("expert"), by_expert)}


def expert_of(by_node, by_expert):
    at = place(by_node, by_expert)
    return at["node"] * 4 + at["expert"]


def one_hot(mask):
    return mask.astype(jnp.float32).astype(jnp.bfloat16)


def matmul(a, b):
    return jnp.dot(a, b, preferred_element_type=jnp.float32)


def matmul_t(a, b):
    return lax.dot_general(a, b, (((0,), (0,)), ((), ())), preferred_element_type=jnp.float32)


def expert_ffn(block, gate_w, up_w, down_w, hidden):
    for start in range(0, hidden.shape[1], FF_TILE):
        cols = slice(start, start + FF_TILE)
        gate = matmul(block, gate_w[:, cols])
        up = matmul(block, up_w[:, cols])
        hidden[:, cols] = (jax.nn.silu(gate) * up).astype(jnp.bfloat16)
    return matmul(hidden[...], down_w[...]).astype(jnp.bfloat16)


def load_weights(refs, scratch, sems):
    loads = [pltpu.make_async_copy(src.at[0], dst, sems.at[i]) for i, (src, dst) in enumerate(zip(refs, scratch))]
    for load in loads:
        load.start()
    return loads


def remote(src, dst, go, come, device):
    return pltpu.make_async_remote_copy(
        src_ref=src, dst_ref=dst, send_sem=go, recv_sem=come, device_id=device, device_id_type=MESH)


def padded_kernel(slot_count, tok_ref, ids_ref, slots_ref, gate_hbm, up_hbm, down_hbm, out_ref,
                  gate_w, up_w, down_w, send, recv, result, back, hidden, total,
                  w_sem, go_sem, come_sem, ret_go_sem, ret_come_sem):
    rows, width = tok_ref.shape
    steps = 16
    loads = load_weights((gate_hbm, up_hbm, down_hbm), (gate_w, up_w, down_w), w_sem)
    barrier = pltpu.get_barrier_semaphore()

    def relative(step):
        far = 1 - step // REMOTE
        return far * (1 + (step % 3 + 1) % 3), far * (step // 3) + (1 - far) * (step - REMOTE)

    def greet(step, carry):
        pl.semaphore_signal(barrier, inc=1, device_id=place(*relative(step)), device_id_type=MESH)
        return carry

    lax.fori_loop(0, REMOTE, greet, 0)
    lax.fori_loop(REMOTE + 1, steps, greet, 0)

    def dispatch_copy(step):
        return remote(send.at[step], recv.at[step], go_sem.at[step], come_sem.at[step], place(*relative(step)))

    def return_copy(step):
        return remote(result.at[step], back.at[step], ret_go_sem.at[step], ret_come_sem.at[step], place(*relative(step)))

    flat_pos = jnp.where(slots_ref[...] >= 0, ids_ref[...] * slot_count + slots_ref[...], steps * slot_count)

    def choice(step):
        first = expert_of(*relative(step)) * slot_count
        return one_hot(flat_pos == lax.broadcasted_iota(jnp.int32, (slot_count, rows), 0) + first)

    def pick(step):
        return matmul(choice(step), tok_ref[...]).astype(jnp.bfloat16)

    pl.semaphore_wait(barrier, steps - 1)

    def dispatch(step, carry):
        send[step] = pick(step)
        dispatch_copy(step).start()
        return carry

    lax.fori_loop(0, REMOTE, dispatch, 0)
    lax.fori_loop(REMOTE + 1, steps, dispatch, 0)
    recv[REMOTE] = pick(REMOTE)
    for load in loads:
        load.wait()

    def compute(order, carry):
        step = (order + REMOTE) % steps

        @pl.when(step != REMOTE)
        def _():
            dispatch_copy(step).wait_recv()

        result[step] = expert_ffn(recv[step], gate_w, up_w, down_w, hidden)

        @pl.when(step != REMOTE)
        def _():
            return_copy(step).start()

        return carry

    lax.fori_loop(0, steps, compute, 0)
    back[REMOTE] = result[REMOTE]
    total[...] = jnp.zeros_like(total)

    def combine(order, carry):
        step = (order + REMOTE) % steps

        @pl.when(step != REMOTE)
        def _():
            return_copy(step).wait_recv()

        total[...] += matmul_t(choice(step), back[step])
        return carry

    lax.fori_loop(0, steps, combine, 0)
    out_ref[...] = total[...].astype(out_ref.dtype)

    def drain(step, carry):
        dispatch_copy(step).wait_send()
        return_copy(step).wait_send()
        return carry

    lax.fori_loop(0, REMOTE, drain, 0)
    lax.fori_loop(REMOTE + 1, steps, drain, 0)


def packed_kernel(slot_count, tok_ref, ids_ref, slots_ref, gate_hbm, up_hbm, down_hbm, out_ref, full_ref,
                  gate_w, up_w, down_w, hidden, total,
                  own_hot, own_send, own_recv, own_result, own_back,
                  z_hot, z_send, z_recv, z_result, z_back,
                  list_hot, list_send, lists, shares, core_in, y_in, z_in, list_back,
                  flag_src, flags, group_src, group_in,
                  w_sem, own_sem, z_sem, list_sem, share_sem, flag_sem):
    rows, width = tok_ref.shape
    node, expert = lax.axis_index("node"), lax.axis_index("expert")
    inner = (node + 1) // 2 == 1
    loads = load_weights((gate_hbm, up_hbm, down_hbm), (gate_w, up_w, down_w), w_sem)

    barrier = pltpu.get_barrier_semaphore()
    twin = {"data": (lax.axis_index("data") + 1) % 2}
    pl.semaphore_signal(barrier, inc=1, device_id=twin, device_id_type=MESH)

    def greet(q, carry):
        pl.semaphore_signal(barrier, inc=1, device_id=place(q // 4, q % 4), device_id_type=MESH)
        return carry

    lax.fori_loop(1, 16, greet, 0)

    def own_copy(w):
        return remote(own_send.at[w], own_recv.at[w], own_sem.at[0, w], own_sem.at[1, w], place(0, w))

    def own_return(w):
        return remote(own_result.at[w], own_back.at[w], own_sem.at[2, w], own_sem.at[3, w], place(0, w))

    def z_part(k):
        return pl.ds(k * BASE, BASE) if k < 2 else pl.ds(2 * BASE, slot_count)

    def z_copy(w, k):
        return remote(z_send.at[w, z_part(k)], z_recv.at[w, z_part(k)], z_sem.at[0, 3 * w + k], z_sem.at[1, 3 * w + k],
                      place((2, 3, 1)[k], w))

    def z_return(w, k):
        return remote(z_result.at[w, z_part(k)], z_back.at[w, z_part(k)], z_sem.at[2, 3 * w + k], z_sem.at[3, 3 * w + k],
                      place((2, 3, 1)[k], w))

    sent = pl.ds(0, LIST)
    gate_node = {"node": 2 - node // 2, "expert": expert}
    kind = 1 - ((node + 1) // 2 + 1) % 2

    def list_out():
        return remote(list_send.at[sent], lists.at[0, kind, sent], list_sem.at[8], list_sem.at[kind], gate_node)

    def forward_z(i):
        return remote(lists.at[0, i, sent], lists.at[0, 1 - i, sent], list_sem.at[9 + i], list_sem.at[1 - i], place(1, 0))

    def forward_y(i):
        return remote(lists.at[0, i, sent], lists.at[2, i, sent], list_sem.at[11 + i], list_sem.at[4 + i], place(0, 2))

    def forward_core(w, i):
        return remote(lists.at[w, i, sent], lists.at[w + 1, i, sent], list_sem.at[13 + w + i], list_sem.at[2 * w + 2 + i],
                      place(0, 1))

    def arrived(w, i):
        return remote(lists.at[w, i, sent], lists.at[w, i, sent], list_sem.at[8], list_sem.at[2 * w + i], place(0, 1))

    def share_core(w, i):
        return remote(shares.at[w, i, sent], core_in.at[w // 2, i, sent], share_sem.at[2 * w + i],
                      share_sem.at[8 + 2 * (w // 2) + i], place(0, 1))

    def share_y(i):
        return remote(shares.at[2, i, sent], y_in.at[i, sent], share_sem.at[4 + i], share_sem.at[12 + i], place(0, 2))

    def share_z(i):
        return remote(shares.at[0, i, sent], z_in.at[1 - i, sent], share_sem.at[i], share_sem.at[15 - i], place(1, 0))

    def share_home(i):
        return remote(shares.at[0, i, sent], list_back.at[sent], share_sem.at[i], share_sem.at[16], place(2 + i, 0))

    def flag_copy(q):
        return remote(flag_src, flags.at[q], flag_sem.at[0, q], flag_sem.at[1, q], place(q // 4, q % 4))

    def group_copy():
        return remote(group_src, group_in, flag_sem.at[0, 0], flag_sem.at[1, 0], twin)

    ids, slots = ids_ref[...], slots_ref[...]
    flat_pos = jnp.where(slots >= 0, ids * slot_count + slots, 16 * slot_count)
    spills = jnp.logical_and(ids // 8 != node // 2, slots >= BASE).astype(jnp.float32)
    lanes = 128
    folds = rows // lanes
    grid = jnp.concatenate([spills[:, i * lanes:(i + 1) * lanes] for i in range(folds)], axis=0)
    upto = one_hot(lax.broadcasted_iota(jnp.int32, (lanes, lanes), 0) <= lax.broadcasted_iota(jnp.int32, (lanes, lanes), 1))
    before = one_hot(lax.broadcasted_iota(jnp.int32, (folds, folds), 1) < lax.broadcasted_iota(jnp.int32, (folds, folds), 0))
    marks = grid.astype(jnp.bfloat16)
    order = matmul(marks, upto) + jnp.sum(matmul(before, marks), axis=1, keepdims=True)
    order = jnp.where(grid > 0, order, 0.0).astype(jnp.int32) - 1
    order = jnp.concatenate([order[i:i + 1, :] for i in range(folds)], axis=1)
    order = jnp.where(order < SPILL, order, -1)
    list_hot[...] = one_hot(order == lax.broadcasted_iota(jnp.int32, (PADDED, rows), 0))
    codes = jnp.concatenate([ids, slots] + [jnp.zeros_like(ids)] * 14, axis=0).astype(jnp.float32).astype(jnp.bfloat16)
    codes = lax.dot_general(codes, list_hot[...], (((1,), (1,)), ((), ())), preferred_element_type=jnp.float32)
    list_send[...] = matmul(list_hot[...], tok_ref[...]).astype(jnp.bfloat16)
    list_send[SPILL:LIST, 0:PADDED] = codes.astype(jnp.bfloat16)
    flag_src[...] = jnp.broadcast_to(jnp.maximum(jnp.sum(spills) - SPILL, 0.0), flag_src.shape)
    for w in range(4):
        for i in range(2):
            lists[w, i, LIST:PADDED] = jnp.zeros((PADDED - LIST, width), jnp.bfloat16)
    list_back[LIST:PADDED] = jnp.zeros((PADDED - LIST, width), jnp.bfloat16)

    pl.semaphore_wait(barrier, 16)
    list_out().start()

    def flag_out(q, carry):
        flag_copy(q).start()
        return carry

    lax.fori_loop(1, 16, flag_out, 0)

    def target(by_node, w, count):
        return lax.broadcasted_iota(jnp.int32, (count, rows), 0) + expert_of(by_node, w) * slot_count

    def own_pick(w, carry):
        own_hot[w] = one_hot(flat_pos == target(0, w, slot_count))
        own_send[w] = matmul(own_hot[w], tok_ref[...]).astype(jnp.bfloat16)

        @pl.when(w > 0)
        def _():
            own_copy(w).start()

        return carry

    def z_pick(w, carry):
        z_hot[w, 0:BASE] = one_hot(flat_pos == target(2, w, BASE))
        z_hot[w, BASE:2 * BASE] = one_hot(flat_pos == target(3, w, BASE))
        z_hot[w, 2 * BASE:] = one_hot(flat_pos == target(1, w, slot_count))
        z_send[w] = matmul(z_hot[w], tok_ref[...]).astype(jnp.bfloat16)
        for k in range(3):
            z_copy(w, k).start()
        return carry

    lax.fori_loop(0, 1, z_pick, 0)
    lax.fori_loop(0, 4, own_pick, 0)
    lax.fori_loop(1, 4, z_pick, 0)
    for load in loads:
        load.wait()

    def ffn(block):
        return expert_ffn(block, gate_w, up_w, down_w, hidden)

    def own_step(w, carry):
        @pl.when(w > 0)
        def _():
            own_copy(w).wait_recv()
            own_result[w] = ffn(own_recv[w])
            own_return(w).start()

        @pl.when(w == 0)
        def _():
            own_back[w] = ffn(own_send[w])

        return carry

    lax.fori_loop(0, 4, own_step, 0)

    def flag_in(q, carry):
        flag_copy(q).wait_recv()
        return carry

    lax.fori_loop(1, 16, flag_in, 0)
    flags[0] = flag_src[...]
    group_src[...] = jnp.max(flags[...], axis=0)

    me = node * 4 + expert

    def round_step(r, carry):
        @pl.when(r == 0)
        def _():
            for i in range(2):
                arrived(0, i).wait_recv()

                @pl.when(inner)
                def _():
                    forward_z(i).start()

                forward_core(0, i).start()
                forward_y(i).start()
            flag_copy(1).wait_send()
            group_copy().start()

        @pl.when(r == 1)
        def _():
            for i in range(2):
                arrived(2, i).wait_recv()
                forward_core(2, i).start()

        z_copy(r, 2).wait_recv()
        near = slice(2 * BASE, 2 * BASE + slot_count)
        far = slice(0, 2 * BASE)
        z_result[r, near] = ffn(z_recv[r, near])
        z_return(r, 2).start()
        z_copy(r, 0).wait_recv()
        z_copy(r, 1).wait_recv()
        z_result[r, far] = ffn(z_recv[r, far])
        z_return(r, 0).start()
        z_return(r, 1).start()

        w = (1 - r // 2) * (2 * r + 1) + (r // 2) * (6 - 2 * r)

        @pl.when(w % 2 == 1)
        def _():
            for i in range(2):
                arrived(w, i).wait_recv()

        mine, blocks = [], []
        for i in range(2):
            codes = lists[w, i, SPILL:LIST, 0:PADDED].astype(jnp.float32)
            slot = lax.broadcasted_iota(jnp.int32, (BASE, PADDED), 0) + BASE
            hit = jnp.logical_and(codes[0:1].astype(jnp.int32) == me, codes[1:2].astype(jnp.int32) == slot)
            mine.append(one_hot(hit))
            blocks.append(matmul(mine[i], lists[w, i]).astype(jnp.bfloat16))
        y = ffn(jnp.concatenate(blocks, axis=0))
        for i in range(2):
            shares[w, i] = matmul_t(mine[i], y[i * BASE:(i + 1) * BASE]).astype(jnp.bfloat16)

        @pl.when(w % 2 == 1)
        def _():
            for i in range(2):
                share_core(w, i).start()

        @pl.when(w == 2)
        def _():
            for i in range(2):
                share_core(3, i).wait_recv()
                shares[2, i, 0:LIST] += core_in[1, i, 0:LIST]
                share_y(i).start()

        return carry

    lax.fori_loop(0, 4, round_step, 0)

    for i in range(2):
        share_core(1, i).wait_recv()
        share_y(i).wait_recv()
        shares[0, i, 0:LIST] += core_in[0, i, 0:LIST] + y_in[i, 0:LIST]

    @pl.when(jnp.logical_not(inner))
    def _():
        for i in range(2):
            share_z(i).start()

    for w in range(1, 4):
        own_return(w).wait_recv()
    total[...] = matmul_t(own_hot[...].reshape(4 * slot_count, rows), own_back[...].reshape(4 * slot_count, width))

    @pl.when(inner)
    def _():
        for i in range(2):
            share_z(1 - i).wait_recv()
            shares[0, i, 0:LIST] += z_in[i, 0:LIST]
            share_home(i).start()

    def z_combine(w, carry):
        for k in (2, 0, 1):
            z_return(w, k).wait_recv()
        total[...] += matmul_t(z_hot[w], z_back[w])
        return carry

    lax.fori_loop(0, 4, z_combine, 0)
    share_home(0).wait_recv()
    total[...] += matmul_t(list_hot[...], list_back[...])
    out_ref[...] = total[...].astype(out_ref.dtype)

    group_copy().wait_recv()
    full_ref[0, 0] = (jnp.max(jnp.maximum(group_src[...], group_in[...])) > 0.0).astype(jnp.int32)

    for w in range(1, 4):
        own_copy(w).wait_send()
        own_return(w).wait_send()
    for w in range(4):
        for k in range(3):
            z_copy(w, k).wait_send()
            z_return(w, k).wait_send()
    list_out().wait_send()
    group_copy().wait_send()

    def flag_sent(q, carry):
        flag_copy(q).wait_send()
        return carry

    lax.fori_loop(2, 16, flag_sent, 0)
    for i in range(2):
        forward_y(i).wait_send()
        forward_core(0, i).wait_send()
        forward_core(2, i).wait_send()
        share_core(1, i).wait_send()
        share_core(3, i).wait_send()
        share_y(i).wait_send()

        @pl.when(inner)
        def _():
            forward_z(i).wait_send()
            share_home(i).wait_send()

        @pl.when(jnp.logical_not(inner))
        def _():
            share_z(i).wait_send()


def solution(mesh):
    group_size = mesh.shape["node"] * mesh.shape["expert"]
    tok_spec = P(("data", "node", "expert"), None)
    weight_spec = P(("node", "expert"), None, None)

    def local_layer(tokens, expert_ids, gate_weights, slot_ids, w_gate, w_up, w_down):
        rows, width = tokens.shape
        ff = w_gate.shape[2]
        slot_count = capacity(rows, 1, group_size)
        vmem = pl.BlockSpec(memory_space=pltpu.VMEM)
        smem = pl.BlockSpec(memory_space=pltpu.SMEM)
        hbm = pl.BlockSpec(memory_space=pl.ANY)
        dma = pltpu.SemaphoreType.DMA
        weights = [pltpu.VMEM((width, ff), jnp.bfloat16), pltpu.VMEM((width, ff), jnp.bfloat16),
                   pltpu.VMEM((ff, width), jnp.bfloat16)]
        hidden = pltpu.VMEM((slot_count, ff), jnp.bfloat16)
        total = pltpu.VMEM((rows, width), jnp.float32)
        picked_shape = jax.ShapeDtypeStruct((rows, width), jnp.bfloat16)
        operands = (tokens, expert_ids.reshape(1, rows), slot_ids.reshape(1, rows), w_gate, w_up, w_down)

        def bf16(*shape):
            return pltpu.VMEM(shape, jnp.bfloat16)

        def params(number):
            return pltpu.CompilerParams(collective_id=number, has_side_effects=True, vmem_limit_bytes=60 * 1024 * 1024)

        def scaled(picked):
            return (gate_weights * picked.astype(jnp.float32)).astype(jnp.bfloat16)

        def padded():
            block = (group_size, slot_count, width)
            return pl.pallas_call(
                functools.partial(padded_kernel, slot_count), out_shape=picked_shape,
                in_specs=[vmem] * 3 + [hbm] * 3, out_specs=vmem,
                scratch_shapes=weights + [bf16(*block)] * 4 + [hidden, total, dma((3,))] + [dma((group_size,))] * 4,
                compiler_params=params(1), name="padded_layer",
            )(*operands)

        own = (4, slot_count, width)
        zed = (4, 2 * BASE + slot_count, width)
        flag = pltpu.VMEM((8, 128), jnp.float32)
        picked, full = pl.pallas_call(
            functools.partial(packed_kernel, slot_count),
            out_shape=(picked_shape, jax.ShapeDtypeStruct((1, 1), jnp.int32)),
            in_specs=[vmem] * 3 + [hbm] * 3, out_specs=(vmem, smem),
            scratch_shapes=weights + [hidden, total]
            + [bf16(4, slot_count, rows)] + [bf16(*own)] * 4
            + [bf16(4, 2 * BASE + slot_count, rows)] + [bf16(*zed)] * 4
            + [bf16(PADDED, rows), bf16(PADDED, width), bf16(4, 2, PADDED, width), bf16(4, 2, PADDED, width),
               bf16(2, 2, PADDED, width), bf16(2, PADDED, width), bf16(2, PADDED, width), bf16(PADDED, width)]
            + [flag, pltpu.VMEM((16, 8, 128), jnp.float32), flag, flag]
            + [dma((3,)), dma((4, 4)), dma((4, 12)), dma((17,)), dma((17,)), dma((2, 16))],
            compiler_params=params(0), name="packed_layer",
        )(*operands)
        return lax.cond(full[0, 0] > 0, lambda: scaled(padded()), lambda: scaled(picked))

    return jax.shard_map(local_layer, mesh=mesh, in_specs=(tok_spec,) * 4 + (weight_spec,) * 3,
                         out_specs=tok_spec, check_vma=False)
```

```python
import functools

import jax
import jax.numpy as jnp
from jax import lax
from jax.experimental import pallas as pl
from jax.experimental.pallas import tpu as pltpu
from jax.sharding import PartitionSpec as P

CAP_FACTOR = 2
MESH = pl.DeviceIdType.MESH
FF_TILE = 512
REMOTE = 12
BASE = 64
SPILL = 144
LIST = SPILL + 16
PADDED = 256


def capacity(rows, top_k, experts):
    return ((CAP_FACTOR * rows * top_k + 8 * experts - 1) // (8 * experts)) * 8


def flip(value, by):
    return 2 * ((value // 2 + by // 2) % 2) + (value + by) % 2


def place(by_node, by_expert):
    return {"node": flip(lax.axis_index("node"), by_node), "expert": flip(lax.axis_index("expert"), by_expert)}


def expert_of(by_node, by_expert):
    at = place(by_node, by_expert)
    return at["node"] * 4 + at["expert"]


def one_hot(mask):
    return mask.astype(jnp.float32).astype(jnp.bfloat16)


def matmul(a, b):
    return jnp.dot(a, b, preferred_element_type=jnp.float32)


def matmul_t(a, b):
    return lax.dot_general(a, b, (((0,), (0,)), ((), ())), preferred_element_type=jnp.float32)


def expert_ffn(block, gate_w, up_w, down_w, hidden):
    for start in range(0, hidden.shape[1], FF_TILE):
        cols = slice(start, start + FF_TILE)
        gate = matmul(block, gate_w[:, cols])
        up = matmul(block, up_w[:, cols])
        hidden[:, cols] = (jax.nn.silu(gate) * up).astype(jnp.bfloat16)
    return matmul(hidden[...], down_w[...]).astype(jnp.bfloat16)


def load_weights(refs, scratch, sems):
    loads = [pltpu.make_async_copy(src.at[0], dst, sems.at[i]) for i, (src, dst) in enumerate(zip(refs, scratch))]
    for load in loads:
        load.start()
    return loads


def remote(src, dst, go, come, device):
    return pltpu.make_async_remote_copy(
        src_ref=src, dst_ref=dst, send_sem=go, recv_sem=come, device_id=device, device_id_type=MESH)


def padded_kernel(slot_count, tok_ref, ids_ref, slots_ref, gate_hbm, up_hbm, down_hbm, out_ref,
                  gate_w, up_w, down_w, send, recv, result, back, hidden, total,
                  w_sem, go_sem, come_sem, ret_go_sem, ret_come_sem):
    rows, width = tok_ref.shape
    steps = 16
    loads = load_weights((gate_hbm, up_hbm, down_hbm), (gate_w, up_w, down_w), w_sem)
    barrier = pltpu.get_barrier_semaphore()

    def relative(step):
        far = 1 - step // REMOTE
        return far * (1 + (step % 3 + 1) % 3), far * (step // 3) + (1 - far) * (step - REMOTE)

    def greet(step, carry):
        pl.semaphore_signal(barrier, inc=1, device_id=place(*relative(step)), device_id_type=MESH)
        return carry

    lax.fori_loop(0, REMOTE, greet, 0)
    lax.fori_loop(REMOTE + 1, steps, greet, 0)

    def dispatch_copy(step):
        return remote(send.at[step], recv.at[step], go_sem.at[step], come_sem.at[step], place(*relative(step)))

    def return_copy(step):
        return remote(result.at[step], back.at[step], ret_go_sem.at[step], ret_come_sem.at[step], place(*relative(step)))

    flat_pos = jnp.where(slots_ref[...] >= 0, ids_ref[...] * slot_count + slots_ref[...], steps * slot_count)

    def choice(step):
        first = expert_of(*relative(step)) * slot_count
        return one_hot(flat_pos == lax.broadcasted_iota(jnp.int32, (slot_count, rows), 0) + first)

    def pick(step):
        return matmul(choice(step), tok_ref[...]).astype(jnp.bfloat16)

    pl.semaphore_wait(barrier, steps - 1)

    def dispatch(step, carry):
        send[step] = pick(step)
        dispatch_copy(step).start()
        return carry

    lax.fori_loop(0, REMOTE, dispatch, 0)
    lax.fori_loop(REMOTE + 1, steps, dispatch, 0)
    recv[REMOTE] = pick(REMOTE)
    for load in loads:
        load.wait()

    def compute(order, carry):
        step = (order + REMOTE) % steps

        @pl.when(step != REMOTE)
        def _():
            dispatch_copy(step).wait_recv()

        result[step] = expert_ffn(recv[step], gate_w, up_w, down_w, hidden)

        @pl.when(step != REMOTE)
        def _():
            return_copy(step).start()

        return carry

    lax.fori_loop(0, steps, compute, 0)
    back[REMOTE] = result[REMOTE]
    total[...] = jnp.zeros_like(total)

    def combine(order, carry):
        step = (order + REMOTE) % steps

        @pl.when(step != REMOTE)
        def _():
            return_copy(step).wait_recv()

        total[...] += matmul_t(choice(step), back[step])
        return carry

    lax.fori_loop(0, steps, combine, 0)
    out_ref[...] = total[...].astype(out_ref.dtype)

    def drain(step, carry):
        dispatch_copy(step).wait_send()
        return_copy(step).wait_send()
        return carry

    lax.fori_loop(0, REMOTE, drain, 0)
    lax.fori_loop(REMOTE + 1, steps, drain, 0)


def packed_kernel(slot_count, tok_ref, ids_ref, slots_ref, gate_hbm, up_hbm, down_hbm, out_ref, full_ref,
                  gate_w, up_w, down_w, hidden, total,
                  own_hot, own_send, own_recv, own_result, own_back,
                  z_hot, z_send, z_recv, z_result, z_back,
                  list_hot, list_send, lists, shares, core_in, z_in, list_back,
                  flag_src, flags, group_src, group_in,
                  w_sem, own_sem, z_sem, list_sem, share_sem, flag_sem):
    rows, width = tok_ref.shape
    node, expert = lax.axis_index("node"), lax.axis_index("expert")
    inner = (node + 1) // 2 == 1
    loads = load_weights((gate_hbm, up_hbm, down_hbm), (gate_w, up_w, down_w), w_sem)

    barrier = pltpu.get_barrier_semaphore()
    twin = {"data": (lax.axis_index("data") + 1) % 2}
    pl.semaphore_signal(barrier, inc=1, device_id=twin, device_id_type=MESH)

    def greet(q, carry):
        pl.semaphore_signal(barrier, inc=1, device_id=place(q // 4, q % 4), device_id_type=MESH)
        return carry

    lax.fori_loop(1, 16, greet, 0)

    def own_copy(w):
        return remote(own_send.at[w], own_recv.at[w], own_sem.at[0, w], own_sem.at[1, w], place(0, w))

    def own_return(w):
        return remote(own_result.at[w], own_back.at[w], own_sem.at[2, w], own_sem.at[3, w], place(0, w))

    def z_part(k):
        return pl.ds(k * BASE, BASE) if k < 2 else pl.ds(2 * BASE, slot_count)

    def z_copy(w, k):
        return remote(z_send.at[w, z_part(k)], z_recv.at[w, z_part(k)], z_sem.at[0, 3 * w + k], z_sem.at[1, 3 * w + k],
                      place((2, 3, 1)[k], w))

    def z_return(w, k):
        return remote(z_result.at[w, z_part(k)], z_back.at[w, z_part(k)], z_sem.at[2, 3 * w + k], z_sem.at[3, 3 * w + k],
                      place((2, 3, 1)[k], w))

    sent = pl.ds(0, LIST)
    kind = 1 - ((node + 1) // 2 + 1) % 2

    def list_out(h):
        return remote(list_send.at[h, sent], lists.at[2 * h, kind, sent], list_sem.at[8 + h], list_sem.at[4 * h + kind],
                      {"node": 2 - node // 2, "expert": flip(expert, 2 * h)})

    def arrived(w, i):
        return remote(lists.at[w, i, sent], lists.at[w, i, sent], list_sem.at[8], list_sem.at[2 * w + i], place(0, 1))

    def forward_z(w, i):
        return remote(lists.at[w, i, sent], lists.at[w, 1 - i, sent], list_sem.at[10 + w + i],
                      list_sem.at[2 * w + 1 - i], place(1, 0))

    def forward_core(w, i):
        return remote(lists.at[w, i, sent], lists.at[w + 1, i, sent], list_sem.at[14 + w + i],
                      list_sem.at[2 * w + 2 + i], place(0, 1))

    def share_core(w, i):
        return remote(shares.at[w, i, sent], core_in.at[w // 2, i, sent], share_sem.at[2 * w + i],
                      share_sem.at[8 + 2 * (w // 2) + i], place(0, 1))

    def share_z(w, i):
        return remote(shares.at[w, i, sent], z_in.at[w // 2, 1 - i, sent], share_sem.at[2 * w + i],
                      share_sem.at[13 + w - i], place(1, 0))

    def share_home(w, i):
        return remote(shares.at[w, i, sent], list_back.at[w // 2, sent], share_sem.at[2 * w + i],
                      share_sem.at[16 + w // 2], place(2 + i, w))

    def flag_copy(q):
        return remote(flag_src, flags.at[q], flag_sem.at[0, q], flag_sem.at[1, q], place(q // 4, q % 4))

    def group_copy():
        return remote(group_src, group_in, flag_sem.at[0, 0], flag_sem.at[1, 0], twin)

    ids, slots = ids_ref[...], slots_ref[...]
    flat_pos = jnp.where(slots >= 0, ids * slot_count + slots, 16 * slot_count)
    far_spill = jnp.logical_and(ids // 8 != node // 2, slots >= BASE)
    lanes = 128
    folds = rows // lanes
    upto = one_hot(lax.broadcasted_iota(jnp.int32, (lanes, lanes), 0) <= lax.broadcasted_iota(jnp.int32, (lanes, lanes), 1))
    before = one_hot(lax.broadcasted_iota(jnp.int32, (folds, folds), 1) < lax.broadcasted_iota(jnp.int32, (folds, folds), 0))
    codes = jnp.concatenate([ids, slots] + [jnp.zeros_like(ids)] * 14, axis=0).astype(jnp.float32).astype(jnp.bfloat16)
    excess = 0.0
    for h in range(2):
        column = (expert // 2 + h) % 2
        spills = jnp.logical_and(far_spill, ids // 2 % 2 == column).astype(jnp.float32)
        grid = jnp.concatenate([spills[:, i * lanes:(i + 1) * lanes] for i in range(folds)], axis=0)
        marks = grid.astype(jnp.bfloat16)
        order = matmul(marks, upto) + jnp.sum(matmul(before, marks), axis=1, keepdims=True)
        order = jnp.where(grid > 0, order, 0.0).astype(jnp.int32) - 1
        order = jnp.concatenate([order[i:i + 1, :] for i in range(folds)], axis=1)
        order = jnp.where(order < SPILL, order, -1)
        list_hot[h] = one_hot(order == lax.broadcasted_iota(jnp.int32, (PADDED, rows), 0))
        named = lax.dot_general(codes, list_hot[h], (((1,), (1,)), ((), ())), preferred_element_type=jnp.float32)
        list_send[h] = matmul(list_hot[h], tok_ref[...]).astype(jnp.bfloat16)
        list_send[h, SPILL:LIST, 0:PADDED] = named.astype(jnp.bfloat16)
        list_back[h, LIST:PADDED] = jnp.zeros((PADDED - LIST, width), jnp.bfloat16)
        excess = jnp.maximum(excess, jnp.sum(spills) - SPILL)
    flag_src[...] = jnp.broadcast_to(excess, flag_src.shape)
    for w in range(4):
        for i in range(2):
            lists[w, i, LIST:PADDED] = jnp.zeros((PADDED - LIST, width), jnp.bfloat16)

    pl.semaphore_wait(barrier, 16)
    list_out(0).start()
    list_out(1).start()

    def flag_out(q, carry):
        flag_copy(q).start()
        return carry

    lax.fori_loop(1, 16, flag_out, 0)

    def target(by_node, w, count):
        return lax.broadcasted_iota(jnp.int32, (count, rows), 0) + expert_of(by_node, w) * slot_count

    def own_pick(w, carry):
        own_hot[w] = one_hot(flat_pos == target(0, w, slot_count))
        own_send[w] = matmul(own_hot[w], tok_ref[...]).astype(jnp.bfloat16)

        @pl.when(w > 0)
        def _():
            own_copy(w).start()

        return carry

    def z_pick(w, carry):
        z_hot[w, 0:BASE] = one_hot(flat_pos == target(2, w, BASE))
        z_hot[w, BASE:2 * BASE] = one_hot(flat_pos == target(3, w, BASE))
        z_hot[w, 2 * BASE:] = one_hot(flat_pos == target(1, w, slot_count))
        z_send[w] = matmul(z_hot[w], tok_ref[...]).astype(jnp.bfloat16)
        z_copy(w, 2).start()
        return carry

    lax.fori_loop(0, 4, own_pick, 0)
    lax.fori_loop(0, 4, z_pick, 0)
    for load in loads:
        load.wait()

    def ffn(block):
        return expert_ffn(block, gate_w, up_w, down_w, hidden)

    own_recv[0] = own_send[0]

    def own_step(w, carry):
        @pl.when(w > 0)
        def _():
            own_copy(w).wait_recv()

        own_result[w] = ffn(own_recv[w])

        @pl.when(w > 0)
        def _():
            own_return(w).start()

        return carry


    me = node * 4 + expert

    near = slice(2 * BASE, 2 * BASE + slot_count)
    far = slice(0, 2 * BASE)

    def near_step(w, carry):
        z_copy(w, 2).wait_recv()
        z_result[w, near] = ffn(z_recv[w, near])

        @pl.when(jnp.logical_not(inner))
        def _():
            z_return(w, 2).start()

        return carry

    def far_step(w, carry):
        z_copy(w, 0).wait_recv()
        z_copy(w, 1).wait_recv()
        z_result[w, far] = ffn(z_recv[w, far])
        z_return(w, 0).start()
        z_return(w, 1).start()
        return carry

    def list_step(r, carry):
        w = (1 - r // 2) * (2 * r + 1) + (r // 2) * (2 * r - 4)

        @pl.when(r < 2)
        def _():
            for i in range(2):
                arrived(w, i).wait_recv()

        mine, blocks = [], []
        for i in range(2):
            codes = lists[w, i, SPILL:LIST, 0:PADDED].astype(jnp.float32)
            slot = lax.broadcasted_iota(jnp.int32, (BASE, PADDED), 0) + BASE
            hit = jnp.logical_and(codes[0:1].astype(jnp.int32) == me, codes[1:2].astype(jnp.int32) == slot)
            mine.append(one_hot(hit))
            blocks.append(matmul(mine[i], lists[w, i]).astype(jnp.bfloat16))
        y = ffn(jnp.concatenate(blocks, axis=0))
        for i in range(2):
            shares[w, i] = matmul_t(mine[i], y[i * BASE:(i + 1) * BASE]).astype(jnp.bfloat16)

        @pl.when(r < 2)
        def _():
            for i in range(2):
                share_core(w, i).start()

        @pl.when(r >= 2)
        def _():
            for i in range(2):
                share_core(w + 1, i).wait_recv()
                shares[w, i, 0:LIST] += core_in[w // 2, i, 0:LIST]

                @pl.when(jnp.logical_not(inner))
                def _():
                    share_z(w, i).start()

        return carry

    def forward_lists():
        for w in (0, 2):
            for i in range(2):
                arrived(w, i).wait_recv()

                @pl.when(inner)
                def _():
                    forward_z(w, i).start()

                forward_core(w, i).start()

    def send_far():
        for w in range(4):
            for k in range(2):
                z_copy(w, k).start()

    def late_step(step, carry):
        turn = step - 2 * (1 - kind)
        lists_now = jnp.logical_and(turn >= 0, turn < 4)
        w = jnp.where(lists_now, turn, jnp.where(turn < 0, step, step - 4))

        @pl.when(jnp.logical_and(step == 2, jnp.logical_not(inner)))
        def _():
            forward_lists()

        @pl.when(jnp.logical_and(step == 4, inner))
        def _():
            for i in range(4):
                z_return(i, 2).start()

        @pl.when(lists_now)
        def _():
            list_step(w, 0)

        @pl.when(jnp.logical_not(lists_now))
        def _():
            far_step(w, 0)

        return carry

    lax.fori_loop(0, 4, own_step, 0)
    own_back[0] = own_result[0]

    @pl.when(inner)
    def _():
        forward_lists()

    send_far()
    lax.fori_loop(0, 4, near_step, 0)
    lax.fori_loop(0, 8, late_step, 0)

    @pl.when(inner)
    def _():
        for w in (0, 2):
            for i in range(2):
                share_z(w, 1 - i).wait_recv()
                shares[w, i, 0:LIST] += z_in[w // 2, i, 0:LIST]
                share_home(w, i).start()

    def flag_in(q, carry):
        flag_copy(q).wait_recv()
        return carry

    lax.fori_loop(1, 16, flag_in, 0)
    flags[0] = flag_src[...]
    group_src[...] = jnp.max(flags[...], axis=0)

    flag_copy(1).wait_send()
    group_copy().start()

    for w in range(1, 4):
        own_return(w).wait_recv()
    total[...] = matmul_t(own_hot[...].reshape(4 * slot_count, rows), own_back[...].reshape(4 * slot_count, width))

    def z_combine(w, carry):
        for k in (2, 0, 1):
            z_return(w, k).wait_recv()
        total[...] += matmul_t(z_hot[w], z_back[w])
        return carry

    lax.fori_loop(0, 4, z_combine, 0)
    for h in range(2):
        share_home(2 * h, 0).wait_recv()
    total[...] += matmul_t(list_hot[...].reshape(2 * PADDED, rows), list_back[...].reshape(2 * PADDED, width))
    out_ref[...] = total[...].astype(out_ref.dtype)

    group_copy().wait_recv()
    full_ref[0, 0] = (jnp.max(jnp.maximum(group_src[...], group_in[...])) > 0.0).astype(jnp.int32)

    for w in range(1, 4):
        own_copy(w).wait_send()
        own_return(w).wait_send()
    for w in range(4):
        for k in range(3):
            z_copy(w, k).wait_send()
            z_return(w, k).wait_send()
    group_copy().wait_send()

    def flag_sent(q, carry):
        flag_copy(q).wait_send()
        return carry

    lax.fori_loop(2, 16, flag_sent, 0)
    for i in range(2):
        list_out(i).wait_send()
        for w in (0, 2):
            forward_core(w, i).wait_send()
            share_core(w + 1, i).wait_send()

            @pl.when(inner)
            def _():
                forward_z(w, i).wait_send()
                share_home(w, i).wait_send()

            @pl.when(jnp.logical_not(inner))
            def _():
                share_z(w, i).wait_send()


def solution(mesh):
    group_size = mesh.shape["node"] * mesh.shape["expert"]
    tok_spec = P(("data", "node", "expert"), None)
    weight_spec = P(("node", "expert"), None, None)

    def local_layer(tokens, expert_ids, gate_weights, slot_ids, w_gate, w_up, w_down):
        rows, width = tokens.shape
        ff = w_gate.shape[2]
        slot_count = capacity(rows, 1, group_size)
        vmem = pl.BlockSpec(memory_space=pltpu.VMEM)
        smem = pl.BlockSpec(memory_space=pltpu.SMEM)
        hbm = pl.BlockSpec(memory_space=pl.ANY)
        dma = pltpu.SemaphoreType.DMA
        weights = [pltpu.VMEM((width, ff), jnp.bfloat16), pltpu.VMEM((width, ff), jnp.bfloat16),
                   pltpu.VMEM((ff, width), jnp.bfloat16)]
        hidden = pltpu.VMEM((slot_count, ff), jnp.bfloat16)
        total = pltpu.VMEM((rows, width), jnp.float32)
        picked_shape = jax.ShapeDtypeStruct((rows, width), jnp.bfloat16)
        operands = (tokens, expert_ids.reshape(1, rows), slot_ids.reshape(1, rows), w_gate, w_up, w_down)

        def bf16(*shape):
            return pltpu.VMEM(shape, jnp.bfloat16)

        def params(number):
            return pltpu.CompilerParams(collective_id=number, has_side_effects=True, vmem_limit_bytes=60 * 1024 * 1024)

        def scaled(picked):
            return (gate_weights * picked.astype(jnp.float32)).astype(jnp.bfloat16)

        def padded():
            block = (group_size, slot_count, width)
            return pl.pallas_call(
                functools.partial(padded_kernel, slot_count), out_shape=picked_shape,
                in_specs=[vmem] * 3 + [hbm] * 3, out_specs=vmem,
                scratch_shapes=weights + [bf16(*block)] * 4 + [hidden, total, dma((3,))] + [dma((group_size,))] * 4,
                compiler_params=params(1), name="padded_layer",
            )(*operands)

        own = (4, slot_count, width)
        zed = (4, 2 * BASE + slot_count, width)
        flag = pltpu.VMEM((8, 128), jnp.float32)
        picked, full = pl.pallas_call(
            functools.partial(packed_kernel, slot_count),
            out_shape=(picked_shape, jax.ShapeDtypeStruct((1, 1), jnp.int32)),
            in_specs=[vmem] * 3 + [hbm] * 3, out_specs=(vmem, smem),
            scratch_shapes=weights + [hidden, total]
            + [bf16(4, slot_count, rows)] + [bf16(*own)] * 4
            + [bf16(4, 2 * BASE + slot_count, rows)] + [bf16(*zed)] * 4
            + [bf16(2, PADDED, rows), bf16(2, PADDED, width), bf16(4, 2, PADDED, width), bf16(4, 2, PADDED, width),
               bf16(2, 2, PADDED, width), bf16(2, 2, PADDED, width), bf16(2, PADDED, width)]
            + [flag, pltpu.VMEM((16, 8, 128), jnp.float32), flag, flag]
            + [dma((3,)), dma((4, 4)), dma((4, 12)), dma((18,)), dma((18,)), dma((2, 16))],
            compiler_params=params(0), name="packed_layer",
        )(*operands)
        return lax.cond(full[0, 0] > 0, lambda: scaled(padded()), lambda: scaled(picked))

    return jax.shard_map(local_layer, mesh=mesh, in_specs=(tok_spec,) * 4 + (weight_spec,) * 3,
                         out_specs=tok_spec, check_vma=False)
```

```python
import functools

import jax
import jax.numpy as jnp
from jax import lax
from jax.experimental import pallas as pl
from jax.experimental.pallas import tpu as pltpu
from jax.sharding import PartitionSpec as P

CAP_FACTOR = 2
MESH = pl.DeviceIdType.MESH
FF_TILE = 512
REMOTE = 12
BASE = 48
SPILL = 160
PADDED = 256
CODES = 16


def capacity(rows, top_k, experts):
    return ((CAP_FACTOR * rows * top_k + 8 * experts - 1) // (8 * experts)) * 8


def flip(value, by):
    return 2 * ((value // 2 + by // 2) % 2) + (value + by) % 2


def place(by_node, by_expert):
    return {"node": flip(lax.axis_index("node"), by_node), "expert": flip(lax.axis_index("expert"), by_expert)}


def expert_of(by_node, by_expert):
    at = place(by_node, by_expert)
    return at["node"] * 4 + at["expert"]


def one_hot(mask):
    return mask.astype(jnp.float32).astype(jnp.bfloat16)


def matmul(a, b):
    return jnp.dot(a, b, preferred_element_type=jnp.float32)


def matmul_t(a, b):
    return lax.dot_general(a, b, (((0,), (0,)), ((), ())), preferred_element_type=jnp.float32)


def expert_ffn(block, gate_w, up_w, down_w, hidden):
    count = block.shape[0]
    for start in range(0, hidden.shape[1], FF_TILE):
        cols = slice(start, start + FF_TILE)
        gate = matmul(block, gate_w[:, cols])
        up = matmul(block, up_w[:, cols])
        hidden[0:count, cols] = (jax.nn.silu(gate) * up).astype(jnp.bfloat16)
    return matmul(hidden[0:count], down_w[...]).astype(jnp.bfloat16)


def load_weights(refs, scratch, sems):
    loads = [pltpu.make_async_copy(src.at[0], dst, sems.at[i]) for i, (src, dst) in enumerate(zip(refs, scratch))]
    for load in loads:
        load.start()
    return loads


def remote(src, dst, go, come, device):
    return pltpu.make_async_remote_copy(
        src_ref=src, dst_ref=dst, send_sem=go, recv_sem=come, device_id=device, device_id_type=MESH)


class Both:
    def __init__(self, first, second):
        self.copies = (first, second)

    def start(self):
        for copy in self.copies:
            copy.start()

    def wait_send(self):
        for copy in self.copies:
            copy.wait_send()

    def wait_recv(self):
        for copy in self.copies:
            copy.wait_recv()


def padded_kernel(slot_count, tok_ref, ids_ref, slots_ref, gate_hbm, up_hbm, down_hbm, out_ref,
                  gate_w, up_w, down_w, send, recv, result, back, hidden, total,
                  w_sem, go_sem, come_sem, ret_go_sem, ret_come_sem):
    rows, width = tok_ref.shape
    steps = 16
    loads = load_weights((gate_hbm, up_hbm, down_hbm), (gate_w, up_w, down_w), w_sem)
    barrier = pltpu.get_barrier_semaphore()

    def relative(step):
        far = 1 - step // REMOTE
        return far * (1 + (step % 3 + 1) % 3), far * (step // 3) + (1 - far) * (step - REMOTE)

    def greet(step, carry):
        pl.semaphore_signal(barrier, inc=1, device_id=place(*relative(step)), device_id_type=MESH)
        return carry

    lax.fori_loop(0, REMOTE, greet, 0)
    lax.fori_loop(REMOTE + 1, steps, greet, 0)

    def dispatch_copy(step):
        return remote(send.at[step], recv.at[step], go_sem.at[step], come_sem.at[step], place(*relative(step)))

    def return_copy(step):
        return remote(result.at[step], back.at[step], ret_go_sem.at[step], ret_come_sem.at[step], place(*relative(step)))

    flat_pos = jnp.where(slots_ref[...] >= 0, ids_ref[...] * slot_count + slots_ref[...], steps * slot_count)

    def choice(step):
        first = expert_of(*relative(step)) * slot_count
        return one_hot(flat_pos == lax.broadcasted_iota(jnp.int32, (slot_count, rows), 0) + first)

    def pick(step):
        return matmul(choice(step), tok_ref[...]).astype(jnp.bfloat16)

    pl.semaphore_wait(barrier, steps - 1)

    def dispatch(step, carry):
        send[step] = pick(step)
        dispatch_copy(step).start()
        return carry

    lax.fori_loop(0, REMOTE, dispatch, 0)
    lax.fori_loop(REMOTE + 1, steps, dispatch, 0)
    recv[REMOTE] = pick(REMOTE)
    for load in loads:
        load.wait()

    def compute(order, carry):
        step = (order + REMOTE) % steps

        @pl.when(step != REMOTE)
        def _():
            dispatch_copy(step).wait_recv()

        result[step] = expert_ffn(recv[step], gate_w, up_w, down_w, hidden)

        @pl.when(step != REMOTE)
        def _():
            return_copy(step).start()

        return carry

    lax.fori_loop(0, steps, compute, 0)
    back[REMOTE] = result[REMOTE]
    total[...] = jnp.zeros_like(total)

    def combine(order, carry):
        step = (order + REMOTE) % steps

        @pl.when(step != REMOTE)
        def _():
            return_copy(step).wait_recv()

        total[...] += matmul_t(choice(step), back[step])
        return carry

    lax.fori_loop(0, steps, combine, 0)
    out_ref[...] = total[...].astype(out_ref.dtype)

    def drain(step, carry):
        dispatch_copy(step).wait_send()
        return_copy(step).wait_send()
        return carry

    lax.fori_loop(0, REMOTE, drain, 0)
    lax.fori_loop(REMOTE + 1, steps, drain, 0)


def packed_kernel(slot_count, tok_ref, ids_ref, slots_ref, gate_hbm, up_hbm, down_hbm, out_ref, full_ref,
                  gate_w, up_w, down_w, hidden, total,
                  own_hot, own_send, own_recv, own_result, own_back,
                  z_hot, z_send, z_recv, z_result, z_back,
                  list_hot, list_send, lists, codes_out, codes_in, shares, core_in, z_in, list_back,
                  flag_src, flags, group_src, group_in,
                  w_sem, own_sem, z_sem, list_sem, code_sem, share_sem, flag_sem):
    rows, width = tok_ref.shape
    node, expert = lax.axis_index("node"), lax.axis_index("expert")
    inner = (node + 1) // 2 == 1
    loads = load_weights((gate_hbm, up_hbm, down_hbm), (gate_w, up_w, down_w), w_sem)

    barrier = pltpu.get_barrier_semaphore()
    twin = {"data": (lax.axis_index("data") + 1) % 2}
    pl.semaphore_signal(barrier, inc=1, device_id=twin, device_id_type=MESH)

    def greet(q, carry):
        pl.semaphore_signal(barrier, inc=1, device_id=place(q // 4, q % 4), device_id_type=MESH)
        return carry

    lax.fori_loop(1, 16, greet, 0)

    def own_copy(w):
        return remote(own_send.at[w], own_recv.at[w], own_sem.at[0, w], own_sem.at[1, w], place(0, w))

    def own_return(w):
        return remote(own_result.at[w], own_back.at[w], own_sem.at[2, w], own_sem.at[3, w], place(0, w))

    def z_part(k):
        return pl.ds(k * BASE, BASE) if k < 2 else pl.ds(2 * BASE, slot_count)

    def z_copy(w, k):
        return remote(z_send.at[w, z_part(k)], z_recv.at[w, z_part(k)], z_sem.at[0, 3 * w + k], z_sem.at[1, 3 * w + k],
                      place((2, 3, 1)[k], w))

    def z_return(w, k):
        return remote(z_result.at[w, z_part(k)], z_back.at[w, z_part(k)], z_sem.at[2, 3 * w + k], z_sem.at[3, 3 * w + k],
                      place((2, 3, 1)[k], w))

    sent = pl.ds(0, SPILL)
    kind = 1 - ((node + 1) // 2 + 1) % 2

    def list_copy(src, codes_src, at, go, device):
        w, i = at
        come = 2 * w + i
        return Both(remote(src.at[sent], lists.at[w, i, sent], list_sem.at[go], list_sem.at[come], device),
                    remote(codes_src, codes_in.at[w, i], code_sem.at[go], code_sem.at[come], device))

    def list_out(h):
        return list_copy(list_send.at[h], codes_out.at[h], (2 * h, kind), 8 + h,
                         {"node": 2 - node // 2, "expert": flip(expert, 2 * h)})

    def arrived(w, i):
        return list_copy(lists.at[w, i], codes_in.at[w, i], (w, i), 8, place(0, 1))

    def forward_z(w, i):
        return list_copy(lists.at[w, i], codes_in.at[w, i], (w, 1 - i), 10 + w + i, place(1, 0))

    def forward_core(w, i):
        return list_copy(lists.at[w, i], codes_in.at[w, i], (w + 1, i), 14 + w + i, place(0, 1))

    def share_core(w, i):
        return remote(shares.at[w, i, sent], core_in.at[w // 2, i, sent], share_sem.at[2 * w + i],
                      share_sem.at[8 + 2 * (w // 2) + i], place(0, 1))

    def share_z(w, i):
        return remote(shares.at[w, i, sent], z_in.at[w // 2, 1 - i, sent], share_sem.at[2 * w + i],
                      share_sem.at[13 + w - i], place(1, 0))

    def share_home(w, i):
        return remote(shares.at[w, i, sent], list_back.at[w // 2, sent], share_sem.at[2 * w + i],
                      share_sem.at[16 + w // 2], place(2 + i, w))

    def flag_copy(q):
        return remote(flag_src, flags.at[q], flag_sem.at[0, q], flag_sem.at[1, q], place(q // 4, q % 4))

    def group_copy():
        return remote(group_src, group_in, flag_sem.at[0, 0], flag_sem.at[1, 0], twin)

    ids, slots = ids_ref[...], slots_ref[...]
    flat_pos = jnp.where(slots >= 0, ids * slot_count + slots, 16 * slot_count)
    far_spill = jnp.logical_and(ids // 8 != node // 2, slots >= BASE)
    lanes = 128
    folds = rows // lanes
    upto = one_hot(lax.broadcasted_iota(jnp.int32, (lanes, lanes), 0) <= lax.broadcasted_iota(jnp.int32, (lanes, lanes), 1))
    before = one_hot(lax.broadcasted_iota(jnp.int32, (folds, folds), 1) < lax.broadcasted_iota(jnp.int32, (folds, folds), 0))
    codes = jnp.concatenate([ids, slots] + [jnp.zeros_like(ids)] * (CODES - 2), axis=0).astype(jnp.float32).astype(jnp.bfloat16)
    excess = 0.0
    for h in range(2):
        column = (expert // 2 + h) % 2
        spills = jnp.logical_and(far_spill, ids // 2 % 2 == column).astype(jnp.float32)
        grid = jnp.concatenate([spills[:, i * lanes:(i + 1) * lanes] for i in range(folds)], axis=0)
        marks = grid.astype(jnp.bfloat16)
        order = matmul(marks, upto) + jnp.sum(matmul(before, marks), axis=1, keepdims=True)
        order = jnp.where(grid > 0, order, 0.0).astype(jnp.int32) - 1
        order = jnp.concatenate([order[i:i + 1, :] for i in range(folds)], axis=1)
        order = jnp.where(order < SPILL, order, -1)
        list_hot[h] = one_hot(order == lax.broadcasted_iota(jnp.int32, (PADDED, rows), 0))
        named = lax.dot_general(codes, list_hot[h], (((1,), (1,)), ((), ())), preferred_element_type=jnp.float32)
        list_send[h] = matmul(list_hot[h], tok_ref[...]).astype(jnp.bfloat16)
        codes_out[h] = named.astype(jnp.bfloat16)
        list_back[h, SPILL:PADDED] = jnp.zeros((PADDED - SPILL, width), jnp.bfloat16)
        excess = jnp.maximum(excess, jnp.sum(spills) - SPILL)
    flag_src[...] = jnp.broadcast_to(excess, flag_src.shape)
    for w in range(4):
        for i in range(2):
            lists[w, i, SPILL:PADDED] = jnp.zeros((PADDED - SPILL, width), jnp.bfloat16)

    pl.semaphore_wait(barrier, 16)
    list_out(0).start()
    list_out(1).start()

    def flag_out(q, carry):
        flag_copy(q).start()
        return carry

    lax.fori_loop(1, 16, flag_out, 0)

    def target(by_node, w, count):
        return lax.broadcasted_iota(jnp.int32, (count, rows), 0) + expert_of(by_node, w) * slot_count

    def own_pick(w, carry):
        own_hot[w] = one_hot(flat_pos == target(0, w, slot_count))
        own_send[w] = matmul(own_hot[w], tok_ref[...]).astype(jnp.bfloat16)

        @pl.when(w > 0)
        def _():
            own_copy(w).start()

        return carry

    def z_pick(w, carry):
        z_hot[w, 0:BASE] = one_hot(flat_pos == target(2, w, BASE))
        z_hot[w, BASE:2 * BASE] = one_hot(flat_pos == target(3, w, BASE))
        z_hot[w, 2 * BASE:] = one_hot(flat_pos == target(1, w, slot_count))
        z_send[w] = matmul(z_hot[w], tok_ref[...]).astype(jnp.bfloat16)
        z_copy(w, 2).start()
        return carry

    lax.fori_loop(0, 4, own_pick, 0)
    lax.fori_loop(0, 4, z_pick, 0)
    for load in loads:
        load.wait()

    def ffn(block):
        return expert_ffn(block, gate_w, up_w, down_w, hidden)

    own_recv[0] = own_send[0]

    def own_step(w, carry):
        @pl.when(w > 0)
        def _():
            own_copy(w).wait_recv()

        own_result[w] = ffn(own_recv[w])

        @pl.when(w > 0)
        def _():
            own_return(w).start()

        return carry


    me = node * 4 + expert
    over = slot_count - BASE

    near = slice(2 * BASE, 2 * BASE + slot_count)
    far = slice(0, 2 * BASE)

    def near_step(w, carry):
        z_copy(w, 2).wait_recv()
        z_result[w, near] = ffn(z_recv[w, near])
        return carry

    def far_step(w, carry):
        z_copy(w, 0).wait_recv()
        z_copy(w, 1).wait_recv()
        z_result[w, far] = ffn(z_recv[w, far])
        z_return(w, 0).start()
        z_return(w, 1).start()
        return carry

    def list_step(r, carry):
        w = r + 1 - 2 * (r % 2)

        @pl.when(r % 2 == 0)
        def _():
            @pl.when(jnp.logical_not(inner))
            def _():
                for i in range(2):
                    arrived(w - 1, i).wait_recv()
                    forward_core(w - 1, i).start()

            for i in range(2):
                arrived(w, i).wait_recv()

        mine, blocks = [], []
        for i in range(2):
            codes = codes_in[w, i].astype(jnp.float32)
            slot = lax.broadcasted_iota(jnp.int32, (over, PADDED), 0) + BASE
            hit = jnp.logical_and(codes[0:1].astype(jnp.int32) == me, codes[1:2].astype(jnp.int32) == slot)
            mine.append(one_hot(hit))
            blocks.append(matmul(mine[i], lists[w, i]).astype(jnp.bfloat16))
        y = ffn(jnp.concatenate(blocks, axis=0))
        for i in range(2):
            shares[w, i] = matmul_t(mine[i], y[i * over:(i + 1) * over]).astype(jnp.bfloat16)

        @pl.when(r % 2 == 0)
        def _():
            for i in range(2):
                share_core(w, i).start()

        @pl.when(r % 2 == 1)
        def _():
            for i in range(2):
                share_core(w + 1, i).wait_recv()
                shares[w, i, 0:SPILL] += core_in[w // 2, i, 0:SPILL]

                @pl.when(jnp.logical_not(inner))
                def _():
                    share_z(w, i).start()

        return carry

    def send_far(first):
        for w in range(4):
            @pl.when(inner)
            def _():
                z_copy(w, first).start()

            @pl.when(jnp.logical_not(inner))
            def _():
                z_copy(w, 1 - first).start()

    lax.fori_loop(0, 4, own_step, 0)
    own_back[0] = own_result[0]

    @pl.when(inner)
    def _():
        for w in (0, 2):
            for i in range(2):
                arrived(w, i).wait_recv()
                forward_core(w, i).start()
                forward_z(w, i).start()

    @pl.when(jnp.logical_not(inner))
    def _():
        send_far(1)

    lax.fori_loop(0, 4, near_step, 0)

    @pl.when(jnp.logical_not(inner))
    def _():
        send_far(0)

    def merge_home(w):
        for i in range(2):
            share_z(w, 1 - i).wait_recv()
            shares[w, i, 0:SPILL] += z_in[w // 2, i, 0:SPILL]
            share_home(w, i).start()

    def late_step(step, carry):
        lists_now = step < 4

        @pl.when(jnp.logical_and(step == 1, inner))
        def _():
            send_far(1)

        @pl.when(jnp.logical_and(step == 3, inner))
        def _():
            send_far(0)

        @pl.when(jnp.logical_and(step == 2, jnp.logical_not(inner)))
        def _():
            for w in range(2):
                z_return(w, 2).start()

        @pl.when(step == 4)
        def _():
            @pl.when(inner)
            def _():
                for w in range(2):
                    z_return(w, 2).start()

            for w in range(2, 4):
                z_return(w, 2).start()

        @pl.when(jnp.logical_and(step == 6, inner))
        def _():
            merge_home(0)

        @pl.when(lists_now)
        def _():
            list_step(step, 0)

        @pl.when(jnp.logical_not(lists_now))
        def _():
            far_step(step - 4, 0)

        return carry

    lax.fori_loop(0, 8, late_step, 0)

    @pl.when(inner)
    def _():
        merge_home(2)

    def flag_in(q, carry):
        flag_copy(q).wait_recv()
        return carry

    lax.fori_loop(1, 16, flag_in, 0)
    flags[0] = flag_src[...]
    group_src[...] = jnp.max(flags[...], axis=0)

    flag_copy(1).wait_send()
    group_copy().start()

    for w in range(1, 4):
        own_return(w).wait_recv()
    total[...] = matmul_t(own_hot[...].reshape(4 * slot_count, rows), own_back[...].reshape(4 * slot_count, width))

    def z_combine(w, carry):
        for k in (2, 0, 1):
            z_return(w, k).wait_recv()
        total[...] += matmul_t(z_hot[w], z_back[w])
        return carry

    lax.fori_loop(0, 4, z_combine, 0)
    for h in range(2):
        share_home(2 * h, 0).wait_recv()
    total[...] += matmul_t(list_hot[...].reshape(2 * PADDED, rows), list_back[...].reshape(2 * PADDED, width))
    out_ref[...] = total[...].astype(out_ref.dtype)

    group_copy().wait_recv()
    full_ref[0, 0] = (jnp.max(jnp.maximum(group_src[...], group_in[...])) > 0.0).astype(jnp.int32)

    for w in range(1, 4):
        own_copy(w).wait_send()
        own_return(w).wait_send()
    for w in range(4):
        for k in range(3):
            z_copy(w, k).wait_send()
            z_return(w, k).wait_send()
    group_copy().wait_send()

    def flag_sent(q, carry):
        flag_copy(q).wait_send()
        return carry

    lax.fori_loop(2, 16, flag_sent, 0)
    for i in range(2):
        list_out(i).wait_send()
        for w in (0, 2):
            forward_core(w, i).wait_send()
            share_core(w + 1, i).wait_send()

            @pl.when(inner)
            def _():
                forward_z(w, i).wait_send()
                share_home(w, i).wait_send()

            @pl.when(jnp.logical_not(inner))
            def _():
                share_z(w, i).wait_send()


def solution(mesh):
    group_size = mesh.shape["node"] * mesh.shape["expert"]
    tok_spec = P(("data", "node", "expert"), None)
    weight_spec = P(("node", "expert"), None, None)

    def local_layer(tokens, expert_ids, gate_weights, slot_ids, w_gate, w_up, w_down):
        rows, width = tokens.shape
        ff = w_gate.shape[2]
        slot_count = capacity(rows, 1, group_size)
        vmem = pl.BlockSpec(memory_space=pltpu.VMEM)
        smem = pl.BlockSpec(memory_space=pltpu.SMEM)
        hbm = pl.BlockSpec(memory_space=pl.ANY)
        dma = pltpu.SemaphoreType.DMA
        weights = [pltpu.VMEM((width, ff), jnp.bfloat16), pltpu.VMEM((width, ff), jnp.bfloat16),
                   pltpu.VMEM((ff, width), jnp.bfloat16)]
        hidden = pltpu.VMEM((2 * (slot_count - BASE), ff), jnp.bfloat16)
        total = pltpu.VMEM((rows, width), jnp.float32)
        picked_shape = jax.ShapeDtypeStruct((rows, width), jnp.bfloat16)
        operands = (tokens, expert_ids.reshape(1, rows), slot_ids.reshape(1, rows), w_gate, w_up, w_down)

        def bf16(*shape):
            return pltpu.VMEM(shape, jnp.bfloat16)

        def params(number):
            return pltpu.CompilerParams(collective_id=number, has_side_effects=True, vmem_limit_bytes=60 * 1024 * 1024)

        def scaled(picked):
            return (gate_weights * picked.astype(jnp.float32)).astype(jnp.bfloat16)

        def padded():
            block = (group_size, slot_count, width)
            return pl.pallas_call(
                functools.partial(padded_kernel, slot_count), out_shape=picked_shape,
                in_specs=[vmem] * 3 + [hbm] * 3, out_specs=vmem,
                scratch_shapes=weights + [bf16(*block)] * 4 + [hidden, total, dma((3,))] + [dma((group_size,))] * 4,
                compiler_params=params(1), name="padded_layer",
            )(*operands)

        own = (4, slot_count, width)
        zed = (4, 2 * BASE + slot_count, width)
        flag = pltpu.VMEM((8, 128), jnp.float32)
        picked, full = pl.pallas_call(
            functools.partial(packed_kernel, slot_count),
            out_shape=(picked_shape, jax.ShapeDtypeStruct((1, 1), jnp.int32)),
            in_specs=[vmem] * 3 + [hbm] * 3, out_specs=(vmem, smem),
            scratch_shapes=weights + [hidden, total]
            + [bf16(4, slot_count, rows)] + [bf16(*own)] * 4
            + [bf16(4, 2 * BASE + slot_count, rows)] + [bf16(*zed)] * 4
            + [bf16(2, PADDED, rows), bf16(2, PADDED, width), bf16(4, 2, PADDED, width),
               bf16(2, CODES, PADDED), bf16(4, 2, CODES, PADDED), bf16(4, 2, PADDED, width),
               bf16(2, 2, PADDED, width), bf16(2, 2, PADDED, width), bf16(2, PADDED, width)]
            + [flag, pltpu.VMEM((16, 8, 128), jnp.float32), flag, flag]
            + [dma((3,)), dma((4, 4)), dma((4, 12)), dma((18,)), dma((18,)), dma((18,)), dma((2, 16))],
            compiler_params=params(0), name="packed_layer",
        )(*operands)
        return lax.cond(full[0, 0] > 0, lambda: scaled(padded()), lambda: scaled(picked))

    return jax.shard_map(local_layer, mesh=mesh, in_specs=(tok_spec,) * 4 + (weight_spec,) * 3,
                         out_specs=tok_spec, check_vma=False)
```

```python
import functools

import jax
import jax.numpy as jnp
from jax import lax
from jax.experimental import pallas as pl
from jax.experimental.pallas import tpu as pltpu
from jax.sharding import PartitionSpec as P

CAP_FACTOR = 2
MESH = pl.DeviceIdType.MESH
FF_TILE = 512
REMOTE = 12
BASE = 48
SPILL = 160
PADDED = 256
CODES = 16
INNER = dict(order="oooollllffffnnnn", near=(0, 0, 0, 0), to_inner=(5, 5, 6, 6), to_outer=(6, 6, 7, 7),
             near_back=(14, 15, 16, 16), home=(11, 16), lists=((0, 0, 4), (0, 1, 4), (2, 0, 4), (2, 1, 4)))
OUTER = dict(order="oooonnnnllllffff", near=(0, 0, 0, 0), to_inner=(4, 4, 4, 4), to_outer=(8, 8, 8, 8),
             near_back=(10, 10, 13, 13))
KINDS = "onfl"


def capacity(rows, top_k, experts):
    return ((CAP_FACTOR * rows * top_k + 8 * experts - 1) // (8 * experts)) * 8


def flip(value, by):
    return 2 * ((value // 2 + by // 2) % 2) + (value + by) % 2


def place(by_node, by_expert):
    return {"node": flip(lax.axis_index("node"), by_node), "expert": flip(lax.axis_index("expert"), by_expert)}


def expert_of(by_node, by_expert):
    at = place(by_node, by_expert)
    return at["node"] * 4 + at["expert"]


def one_hot(mask):
    return mask.astype(jnp.float32).astype(jnp.bfloat16)


def matmul(a, b):
    return jnp.dot(a, b, preferred_element_type=jnp.float32)


def matmul_t(a, b):
    return lax.dot_general(a, b, (((0,), (0,)), ((), ())), preferred_element_type=jnp.float32)


def expert_ffn(block, gate_w, up_w, down_w, hidden):
    count = block.shape[0]
    for start in range(0, hidden.shape[1], FF_TILE):
        cols = slice(start, start + FF_TILE)
        gate = matmul(block, gate_w[:, cols])
        up = matmul(block, up_w[:, cols])
        hidden[0:count, cols] = (jax.nn.silu(gate) * up).astype(jnp.bfloat16)
    return matmul(hidden[0:count], down_w[...]).astype(jnp.bfloat16)


def load_weights(refs, scratch, sems):
    loads = [pltpu.make_async_copy(src.at[0], dst, sems.at[i]) for i, (src, dst) in enumerate(zip(refs, scratch))]
    for load in loads:
        load.start()
    return loads


def remote(src, dst, go, come, device):
    return pltpu.make_async_remote_copy(
        src_ref=src, dst_ref=dst, send_sem=go, recv_sem=come, device_id=device, device_id_type=MESH)


class Both:
    def __init__(self, first, second):
        self.copies = (first, second)

    def start(self):
        for copy in self.copies:
            copy.start()

    def wait_send(self):
        for copy in self.copies:
            copy.wait_send()

    def wait_recv(self):
        for copy in self.copies:
            copy.wait_recv()


def padded_kernel(slot_count, tok_ref, ids_ref, slots_ref, gate_hbm, up_hbm, down_hbm, out_ref,
                  gate_w, up_w, down_w, send, recv, result, back, hidden, total,
                  w_sem, go_sem, come_sem, ret_go_sem, ret_come_sem):
    rows, width = tok_ref.shape
    steps = 16
    loads = load_weights((gate_hbm, up_hbm, down_hbm), (gate_w, up_w, down_w), w_sem)
    barrier = pltpu.get_barrier_semaphore()

    def relative(step):
        far = 1 - step // REMOTE
        return far * (1 + (step % 3 + 1) % 3), far * (step // 3) + (1 - far) * (step - REMOTE)

    def greet(step, carry):
        pl.semaphore_signal(barrier, inc=1, device_id=place(*relative(step)), device_id_type=MESH)
        return carry

    lax.fori_loop(0, REMOTE, greet, 0)
    lax.fori_loop(REMOTE + 1, steps, greet, 0)

    def dispatch_copy(step):
        return remote(send.at[step], recv.at[step], go_sem.at[step], come_sem.at[step], place(*relative(step)))

    def return_copy(step):
        return remote(result.at[step], back.at[step], ret_go_sem.at[step], ret_come_sem.at[step], place(*relative(step)))

    flat_pos = jnp.where(slots_ref[...] >= 0, ids_ref[...] * slot_count + slots_ref[...], steps * slot_count)

    def choice(step):
        first = expert_of(*relative(step)) * slot_count
        return one_hot(flat_pos == lax.broadcasted_iota(jnp.int32, (slot_count, rows), 0) + first)

    def pick(step):
        return matmul(choice(step), tok_ref[...]).astype(jnp.bfloat16)

    pl.semaphore_wait(barrier, steps - 1)

    def dispatch(step, carry):
        send[step] = pick(step)
        dispatch_copy(step).start()
        return carry

    lax.fori_loop(0, REMOTE, dispatch, 0)
    lax.fori_loop(REMOTE + 1, steps, dispatch, 0)
    recv[REMOTE] = pick(REMOTE)
    for load in loads:
        load.wait()

    def compute(order, carry):
        step = (order + REMOTE) % steps

        @pl.when(step != REMOTE)
        def _():
            dispatch_copy(step).wait_recv()

        result[step] = expert_ffn(recv[step], gate_w, up_w, down_w, hidden)

        @pl.when(step != REMOTE)
        def _():
            return_copy(step).start()

        return carry

    lax.fori_loop(0, steps, compute, 0)
    back[REMOTE] = result[REMOTE]
    total[...] = jnp.zeros_like(total)

    def combine(order, carry):
        step = (order + REMOTE) % steps

        @pl.when(step != REMOTE)
        def _():
            return_copy(step).wait_recv()

        total[...] += matmul_t(choice(step), back[step])
        return carry

    lax.fori_loop(0, steps, combine, 0)
    out_ref[...] = total[...].astype(out_ref.dtype)

    def drain(step, carry):
        dispatch_copy(step).wait_send()
        return_copy(step).wait_send()
        return carry

    lax.fori_loop(0, REMOTE, drain, 0)
    lax.fori_loop(REMOTE + 1, steps, drain, 0)


def packed_kernel(slot_count, tok_ref, ids_ref, slots_ref, gate_hbm, up_hbm, down_hbm, out_ref, full_ref,
                  gate_w, up_w, down_w, hidden, total,
                  own_hot, own_send, own_recv, own_result, own_back,
                  z_hot, z_send, z_recv, z_result, z_back,
                  list_hot, list_send, lists, codes_out, codes_in, shares, core_in, z_in, list_back,
                  flag_src, flags, group_src, group_in,
                  w_sem, own_sem, z_sem, list_sem, code_sem, share_sem, flag_sem):
    rows, width = tok_ref.shape
    node, expert = lax.axis_index("node"), lax.axis_index("expert")
    inner = (node + 1) // 2 == 1
    roles = ((INNER, inner), (OUTER, jnp.logical_not(inner)))
    loads = load_weights((gate_hbm, up_hbm, down_hbm), (gate_w, up_w, down_w), w_sem)

    barrier = pltpu.get_barrier_semaphore()
    twin = {"data": (lax.axis_index("data") + 1) % 2}
    pl.semaphore_signal(barrier, inc=1, device_id=twin, device_id_type=MESH)

    def greet(q, carry):
        pl.semaphore_signal(barrier, inc=1, device_id=place(q // 4, q % 4), device_id_type=MESH)
        return carry

    lax.fori_loop(1, 16, greet, 0)

    def own_copy(w):
        return remote(own_send.at[w], own_recv.at[w], own_sem.at[0, w], own_sem.at[1, w], place(0, w))

    def own_return(w):
        return remote(own_result.at[w], own_back.at[w], own_sem.at[2, w], own_sem.at[3, w], place(0, w))

    def z_part(k):
        return pl.ds(k * BASE, BASE) if k < 2 else pl.ds(2 * BASE, slot_count)

    def z_copy(w, k):
        return remote(z_send.at[w, z_part(k)], z_recv.at[w, z_part(k)], z_sem.at[0, 3 * w + k], z_sem.at[1, 3 * w + k],
                      place((2, 3, 1)[k], w))

    def z_return(w, k):
        return remote(z_result.at[w, z_part(k)], z_back.at[w, z_part(k)], z_sem.at[2, 3 * w + k], z_sem.at[3, 3 * w + k],
                      place((2, 3, 1)[k], w))

    sent = pl.ds(0, SPILL)
    kind = 1 - ((node + 1) // 2 + 1) % 2

    def list_copy(src, codes_src, at, go, device):
        w, i = at
        come = 2 * w + i
        return Both(remote(src.at[sent], lists.at[w, i, sent], list_sem.at[go], list_sem.at[come], device),
                    remote(codes_src, codes_in.at[w, i], code_sem.at[go], code_sem.at[come], device))

    def list_out(h):
        return list_copy(list_send.at[h], codes_out.at[h], (2 * h, kind), 8 + h,
                         {"node": 2 - node // 2, "expert": flip(expert, 2 * h)})

    def arrived(w, i):
        return list_copy(lists.at[w, i], codes_in.at[w, i], (w, i), 8, place(0, 1))

    def forward_z(w, i):
        return list_copy(lists.at[w, i], codes_in.at[w, i], (w, 1 - i), 10 + w + i, place(1, 0))

    def forward_core(w, i):
        return list_copy(lists.at[w, i], codes_in.at[w, i], (w + 1, i), 14 + w + i, place(0, 1))

    def share_core(w, i):
        return remote(shares.at[w, i, sent], core_in.at[w // 2, i, sent], share_sem.at[2 * w + i],
                      share_sem.at[8 + 2 * (w // 2) + i], place(0, 1))

    def share_z(w, i):
        return remote(shares.at[w, i, sent], z_in.at[w // 2, 1 - i, sent], share_sem.at[2 * w + i],
                      share_sem.at[13 + w - i], place(1, 0))

    def share_home(w, i):
        return remote(shares.at[w, i, sent], list_back.at[w // 2, sent], share_sem.at[2 * w + i],
                      share_sem.at[16 + w // 2], place(2 + i, w))

    def flag_copy(q):
        return remote(flag_src, flags.at[q], flag_sem.at[0, q], flag_sem.at[1, q], place(q // 4, q % 4))

    def group_copy():
        return remote(group_src, group_in, flag_sem.at[0, 0], flag_sem.at[1, 0], twin)

    ids, slots = ids_ref[...], slots_ref[...]
    flat_pos = jnp.where(slots >= 0, ids * slot_count + slots, 16 * slot_count)
    far_spill = jnp.logical_and(ids // 8 != node // 2, slots >= BASE)
    lanes = 128
    folds = rows // lanes
    upto = one_hot(lax.broadcasted_iota(jnp.int32, (lanes, lanes), 0) <= lax.broadcasted_iota(jnp.int32, (lanes, lanes), 1))
    before = one_hot(lax.broadcasted_iota(jnp.int32, (folds, folds), 1) < lax.broadcasted_iota(jnp.int32, (folds, folds), 0))
    codes = jnp.concatenate([ids, slots] + [jnp.zeros_like(ids)] * (CODES - 2), axis=0).astype(jnp.float32).astype(jnp.bfloat16)
    excess = 0.0
    for h in range(2):
        column = (expert // 2 + h) % 2
        spills = jnp.logical_and(far_spill, ids // 2 % 2 == column).astype(jnp.float32)
        grid = jnp.concatenate([spills[:, i * lanes:(i + 1) * lanes] for i in range(folds)], axis=0)
        marks = grid.astype(jnp.bfloat16)
        order = matmul(marks, upto) + jnp.sum(matmul(before, marks), axis=1, keepdims=True)
        order = jnp.where(grid > 0, order, 0.0).astype(jnp.int32) - 1
        order = jnp.concatenate([order[i:i + 1, :] for i in range(folds)], axis=1)
        order = jnp.where(order < SPILL, order, -1)
        list_hot[h] = one_hot(order == lax.broadcasted_iota(jnp.int32, (PADDED, rows), 0))
        named = lax.dot_general(codes, list_hot[h], (((1,), (1,)), ((), ())), preferred_element_type=jnp.float32)
        list_send[h] = matmul(list_hot[h], tok_ref[...]).astype(jnp.bfloat16)
        codes_out[h] = named.astype(jnp.bfloat16)
        list_back[h, SPILL:PADDED] = jnp.zeros((PADDED - SPILL, width), jnp.bfloat16)
        excess = jnp.maximum(excess, jnp.sum(spills) - SPILL)
    flag_src[...] = jnp.broadcast_to(excess, flag_src.shape)
    for w in range(4):
        for i in range(2):
            lists[w, i, SPILL:PADDED] = jnp.zeros((PADDED - SPILL, width), jnp.bfloat16)

    pl.semaphore_wait(barrier, 16)
    list_out(0).start()
    list_out(1).start()

    def flag_out(q, carry):
        flag_copy(q).start()
        return carry

    lax.fori_loop(1, 16, flag_out, 0)

    def target(by_node, w, count):
        return lax.broadcasted_iota(jnp.int32, (count, rows), 0) + expert_of(by_node, w) * slot_count

    def own_pick(w, carry):
        own_hot[w] = one_hot(flat_pos == target(0, w, slot_count))
        own_send[w] = matmul(own_hot[w], tok_ref[...]).astype(jnp.bfloat16)

        @pl.when(w > 0)
        def _():
            own_copy(w).start()

        return carry

    def z_pick(w, carry):
        z_hot[w, 0:BASE] = one_hot(flat_pos == target(2, w, BASE))
        z_hot[w, BASE:2 * BASE] = one_hot(flat_pos == target(3, w, BASE))
        z_hot[w, 2 * BASE:] = one_hot(flat_pos == target(1, w, slot_count))
        z_send[w] = matmul(z_hot[w], tok_ref[...]).astype(jnp.bfloat16)

        for role, is_role in roles:
            early = [v for v in range(4) if role["near"][v] == 0]
            if early == [0, 1, 2, 3]:
                @pl.when(is_role)
                def _():
                    z_copy(w, 2).start()

        return carry

    lax.fori_loop(0, 4, own_pick, 0)
    lax.fori_loop(0, 4, z_pick, 0)
    for load in loads:
        load.wait()

    def ffn(block):
        return expert_ffn(block, gate_w, up_w, down_w, hidden)

    own_recv[0] = own_send[0]

    def own_step(w, carry):
        @pl.when(w > 0)
        def _():
            own_copy(w).wait_recv()

        own_result[w] = ffn(own_recv[w])

        @pl.when(w > 0)
        def _():
            own_return(w).start()

        return carry


    me = node * 4 + expert
    over = slot_count - BASE

    near = slice(2 * BASE, 2 * BASE + slot_count)
    far = slice(0, 2 * BASE)

    def near_step(w, carry):
        z_copy(w, 2).wait_recv()
        z_result[w, near] = ffn(z_recv[w, near])
        return carry

    def far_step(w, carry):
        z_copy(w, 0).wait_recv()
        z_copy(w, 1).wait_recv()
        z_result[w, far] = ffn(z_recv[w, far])
        z_return(w, 0).start()
        z_return(w, 1).start()
        return carry

    def list_step(r, carry):
        w = r + 1 - 2 * (r % 2)

        @pl.when(r % 2 == 0)
        def _():
            @pl.when(jnp.logical_not(inner))
            def _():
                for i in range(2):
                    arrived(w - 1, i).wait_recv()
                    forward_core(w - 1, i).start()

            for i in range(2):
                arrived(w, i).wait_recv()

        mine, blocks = [], []
        for i in range(2):
            codes = codes_in[w, i].astype(jnp.float32)
            slot = lax.broadcasted_iota(jnp.int32, (over, PADDED), 0) + BASE
            hit = jnp.logical_and(codes[0:1].astype(jnp.int32) == me, codes[1:2].astype(jnp.int32) == slot)
            mine.append(one_hot(hit))
            blocks.append(matmul(mine[i], lists[w, i]).astype(jnp.bfloat16))
        y = ffn(jnp.concatenate(blocks, axis=0))
        for i in range(2):
            shares[w, i] = matmul_t(mine[i], y[i * over:(i + 1) * over]).astype(jnp.bfloat16)

        @pl.when(r % 2 == 0)
        def _():
            for i in range(2):
                share_core(w, i).start()

        @pl.when(r % 2 == 1)
        def _():
            for i in range(2):
                share_core(w + 1, i).wait_recv()
                shares[w, i, 0:SPILL] += core_in[w // 2, i, 0:SPILL]

                @pl.when(jnp.logical_not(inner))
                def _():
                    share_z(w, i).start()

        return carry

    def forward_list(w, i):
        arrived(w, i).wait_recv()
        forward_core(w, i).start()
        forward_z(w, i).start()

    def merge_home(w):
        for i in range(2):
            share_z(w, 1 - i).wait_recv()
            shares[w, i, 0:SPILL] += z_in[w // 2, i, 0:SPILL]
            share_home(w, i).start()

    def acts(role, slot):
        same = kind_of_far[role is INNER]
        found = []
        for w in range(4):
            if role["near"][w] == slot and role["near"] != (0, 0, 0, 0):
                found.append(z_copy(w, 2).start)
        for name, k in (("to_inner", same), ("to_outer", 1 - same)):
            found += [z_copy(w, k).start for w in range(4) if role[name][w] == slot]
        found += [z_return(w, 2).start for w in range(4) if role["near_back"][w] == slot]
        if role is INNER:
            found += [functools.partial(forward_list, w, i) for w, i, when in role["lists"] if when == slot]
            found += [functools.partial(merge_home, w) for w in (0, 2) if role["home"][w // 2] == slot]
        return found

    kind_of_far = {True: 1, False: 0}

    def fire(at):
        for role, is_role in roles:
            for slot in range(len(role["order"])):
                todo = acts(role, slot)
                if todo:
                    @pl.when(jnp.logical_and(at == slot, is_role))
                    def _():
                        for act in todo:
                            act()

    def table(values, at):
        inner_values, outer_values = values
        total = 0
        for slot, (a, b) in enumerate(zip(inner_values, outer_values)):
            total = total + jnp.where(at == slot, a if a == b else jnp.where(inner, a, b), 0)
        return total

    orders = [role["order"] for role, _ in roles]
    sorts = [[KINDS.index(letter) for letter in order] for order in orders]
    turns = [[order[:slot].count(letter) for slot, letter in enumerate(order)] for order in orders]

    def slot_step(at, carry):
        fire(at)
        sort, turn = table(sorts, at), table(turns, at)
        for number, step in enumerate((own_step, near_step, far_step, list_step)):
            @pl.when(sort == number)
            def _():
                step(turn, 0)

        return carry

    lax.fori_loop(0, 16, slot_step, 0)
    own_back[0] = own_result[0]
    for role, is_role in roles:
        todo = acts(role, 16)
        if todo:
            @pl.when(is_role)
            def _():
                for act in todo:
                    act()

    def flag_in(q, carry):
        flag_copy(q).wait_recv()
        return carry

    lax.fori_loop(1, 16, flag_in, 0)
    flags[0] = flag_src[...]
    group_src[...] = jnp.max(flags[...], axis=0)

    flag_copy(1).wait_send()
    group_copy().start()

    for w in range(1, 4):
        own_return(w).wait_recv()
    total[...] = matmul_t(own_hot[...].reshape(4 * slot_count, rows), own_back[...].reshape(4 * slot_count, width))

    def z_combine(w, carry):
        for k in (2, 0, 1):
            z_return(w, k).wait_recv()
        total[...] += matmul_t(z_hot[w], z_back[w])
        return carry

    lax.fori_loop(0, 4, z_combine, 0)
    for h in range(2):
        share_home(2 * h, 0).wait_recv()
    total[...] += matmul_t(list_hot[...].reshape(2 * PADDED, rows), list_back[...].reshape(2 * PADDED, width))
    out_ref[...] = total[...].astype(out_ref.dtype)

    group_copy().wait_recv()
    full_ref[0, 0] = (jnp.max(jnp.maximum(group_src[...], group_in[...])) > 0.0).astype(jnp.int32)

    for w in range(1, 4):
        own_copy(w).wait_send()
        own_return(w).wait_send()
    for w in range(4):
        for k in range(3):
            z_copy(w, k).wait_send()
            z_return(w, k).wait_send()
    group_copy().wait_send()

    def flag_sent(q, carry):
        flag_copy(q).wait_send()
        return carry

    lax.fori_loop(2, 16, flag_sent, 0)
    for i in range(2):
        list_out(i).wait_send()
        for w in (0, 2):
            forward_core(w, i).wait_send()
            share_core(w + 1, i).wait_send()

            @pl.when(inner)
            def _():
                forward_z(w, i).wait_send()
                share_home(w, i).wait_send()

            @pl.when(jnp.logical_not(inner))
            def _():
                share_z(w, i).wait_send()


def solution(mesh):
    group_size = mesh.shape["node"] * mesh.shape["expert"]
    tok_spec = P(("data", "node", "expert"), None)
    weight_spec = P(("node", "expert"), None, None)

    def local_layer(tokens, expert_ids, gate_weights, slot_ids, w_gate, w_up, w_down):
        rows, width = tokens.shape
        ff = w_gate.shape[2]
        slot_count = capacity(rows, 1, group_size)
        vmem = pl.BlockSpec(memory_space=pltpu.VMEM)
        smem = pl.BlockSpec(memory_space=pltpu.SMEM)
        hbm = pl.BlockSpec(memory_space=pl.ANY)
        dma = pltpu.SemaphoreType.DMA
        weights = [pltpu.VMEM((width, ff), jnp.bfloat16), pltpu.VMEM((width, ff), jnp.bfloat16),
                   pltpu.VMEM((ff, width), jnp.bfloat16)]
        hidden = pltpu.VMEM((2 * (slot_count - BASE), ff), jnp.bfloat16)
        total = pltpu.VMEM((rows, width), jnp.float32)
        picked_shape = jax.ShapeDtypeStruct((rows, width), jnp.bfloat16)
        operands = (tokens, expert_ids.reshape(1, rows), slot_ids.reshape(1, rows), w_gate, w_up, w_down)

        def bf16(*shape):
            return pltpu.VMEM(shape, jnp.bfloat16)

        def params(number):
            return pltpu.CompilerParams(collective_id=number, has_side_effects=True, vmem_limit_bytes=60 * 1024 * 1024)

        def scaled(picked):
            return (gate_weights * picked.astype(jnp.float32)).astype(jnp.bfloat16)

        def padded():
            block = (group_size, slot_count, width)
            return pl.pallas_call(
                functools.partial(padded_kernel, slot_count), out_shape=picked_shape,
                in_specs=[vmem] * 3 + [hbm] * 3, out_specs=vmem,
                scratch_shapes=weights + [bf16(*block)] * 4 + [hidden, total, dma((3,))] + [dma((group_size,))] * 4,
                compiler_params=params(1), name="padded_layer",
            )(*operands)

        own = (4, slot_count, width)
        zed = (4, 2 * BASE + slot_count, width)
        flag = pltpu.VMEM((8, 128), jnp.float32)
        picked, full = pl.pallas_call(
            functools.partial(packed_kernel, slot_count),
            out_shape=(picked_shape, jax.ShapeDtypeStruct((1, 1), jnp.int32)),
            in_specs=[vmem] * 3 + [hbm] * 3, out_specs=(vmem, smem),
            scratch_shapes=weights + [hidden, total]
            + [bf16(4, slot_count, rows)] + [bf16(*own)] * 4
            + [bf16(4, 2 * BASE + slot_count, rows)] + [bf16(*zed)] * 4
            + [bf16(2, PADDED, rows), bf16(2, PADDED, width), bf16(4, 2, PADDED, width),
               bf16(2, CODES, PADDED), bf16(4, 2, CODES, PADDED), bf16(4, 2, PADDED, width),
               bf16(2, 2, PADDED, width), bf16(2, 2, PADDED, width), bf16(2, PADDED, width)]
            + [flag, pltpu.VMEM((16, 8, 128), jnp.float32), flag, flag]
            + [dma((3,)), dma((4, 4)), dma((4, 12)), dma((18,)), dma((18,)), dma((18,)), dma((2, 16))],
            compiler_params=params(0), name="packed_layer",
        )(*operands)
        return lax.cond(full[0, 0] > 0, lambda: scaled(padded()), lambda: scaled(picked))

    return jax.shard_map(local_layer, mesh=mesh, in_specs=(tok_spec,) * 4 + (weight_spec,) * 3,
                         out_specs=tok_spec, check_vma=False)
```

```python
import functools

import jax
import jax.numpy as jnp
from jax import lax
from jax.experimental import pallas as pl
from jax.experimental.pallas import tpu as pltpu
from jax.sharding import PartitionSpec as P

CAP_FACTOR = 2
MESH = pl.DeviceIdType.MESH
FF_TILE = 512
REMOTE = 12
BASE = 48
SPILL = 160
PADDED = 256
CODES = 16
INNER = dict(order="oolollloffffnnnn", near=(0, 0, 0, 0), to_inner=(3, 3, 4, 4), to_outer=(5, 5, 6, 6),
             near_back=(14, 15, 16, 16), home=(12, 16), lists=((0, 0, 2), (0, 1, 2), (2, 0, 2), (2, 1, 2)))
OUTER = dict(order="oooonnnnllllffff", near=(0, 0, 0, 0), to_inner=(4, 4, 4, 4), to_outer=(8, 8, 8, 8),
             near_back=(10, 10, 13, 13))
KINDS = "onfl"


def capacity(rows, top_k, experts):
    return ((CAP_FACTOR * rows * top_k + 8 * experts - 1) // (8 * experts)) * 8


def flip(value, by):
    return 2 * ((value // 2 + by // 2) % 2) + (value + by) % 2


def place(by_node, by_expert):
    return {"node": flip(lax.axis_index("node"), by_node), "expert": flip(lax.axis_index("expert"), by_expert)}


def expert_of(by_node, by_expert):
    at = place(by_node, by_expert)
    return at["node"] * 4 + at["expert"]


def one_hot(mask):
    return mask.astype(jnp.float32).astype(jnp.bfloat16)


def matmul(a, b):
    return jnp.dot(a, b, preferred_element_type=jnp.float32)


def matmul_t(a, b):
    return lax.dot_general(a, b, (((0,), (0,)), ((), ())), preferred_element_type=jnp.float32)


def expert_ffn(block, gate_w, up_w, down_w, hidden):
    count = block.shape[0]
    for start in range(0, hidden.shape[1], FF_TILE):
        cols = slice(start, start + FF_TILE)
        gate = matmul(block, gate_w[:, cols])
        up = matmul(block, up_w[:, cols])
        hidden[0:count, cols] = (jax.nn.silu(gate) * up).astype(jnp.bfloat16)
    return matmul(hidden[0:count], down_w[...]).astype(jnp.bfloat16)


def load_weights(refs, scratch, sems):
    loads = [pltpu.make_async_copy(src.at[0], dst, sems.at[i]) for i, (src, dst) in enumerate(zip(refs, scratch))]
    for load in loads:
        load.start()
    return loads


def remote(src, dst, go, come, device):
    return pltpu.make_async_remote_copy(
        src_ref=src, dst_ref=dst, send_sem=go, recv_sem=come, device_id=device, device_id_type=MESH)


class Both:
    def __init__(self, first, second):
        self.copies = (first, second)

    def start(self):
        for copy in self.copies:
            copy.start()

    def wait_send(self):
        for copy in self.copies:
            copy.wait_send()

    def wait_recv(self):
        for copy in self.copies:
            copy.wait_recv()


def padded_kernel(slot_count, tok_ref, ids_ref, slots_ref, gate_hbm, up_hbm, down_hbm, out_ref,
                  gate_w, up_w, down_w, send, recv, result, back, hidden, total,
                  w_sem, go_sem, come_sem, ret_go_sem, ret_come_sem):
    rows, width = tok_ref.shape
    steps = 16
    loads = load_weights((gate_hbm, up_hbm, down_hbm), (gate_w, up_w, down_w), w_sem)
    barrier = pltpu.get_barrier_semaphore()

    def relative(step):
        far = 1 - step // REMOTE
        return far * (1 + (step % 3 + 1) % 3), far * (step // 3) + (1 - far) * (step - REMOTE)

    def greet(step, carry):
        pl.semaphore_signal(barrier, inc=1, device_id=place(*relative(step)), device_id_type=MESH)
        return carry

    lax.fori_loop(0, REMOTE, greet, 0)
    lax.fori_loop(REMOTE + 1, steps, greet, 0)

    def dispatch_copy(step):
        return remote(send.at[step], recv.at[step], go_sem.at[step], come_sem.at[step], place(*relative(step)))

    def return_copy(step):
        return remote(result.at[step], back.at[step], ret_go_sem.at[step], ret_come_sem.at[step], place(*relative(step)))

    flat_pos = jnp.where(slots_ref[...] >= 0, ids_ref[...] * slot_count + slots_ref[...], steps * slot_count)

    def choice(step):
        first = expert_of(*relative(step)) * slot_count
        return one_hot(flat_pos == lax.broadcasted_iota(jnp.int32, (slot_count, rows), 0) + first)

    def pick(step):
        return matmul(choice(step), tok_ref[...]).astype(jnp.bfloat16)

    pl.semaphore_wait(barrier, steps - 1)

    def dispatch(step, carry):
        send[step] = pick(step)
        dispatch_copy(step).start()
        return carry

    lax.fori_loop(0, REMOTE, dispatch, 0)
    lax.fori_loop(REMOTE + 1, steps, dispatch, 0)
    recv[REMOTE] = pick(REMOTE)
    for load in loads:
        load.wait()

    def compute(order, carry):
        step = (order + REMOTE) % steps

        @pl.when(step != REMOTE)
        def _():
            dispatch_copy(step).wait_recv()

        result[step] = expert_ffn(recv[step], gate_w, up_w, down_w, hidden)

        @pl.when(step != REMOTE)
        def _():
            return_copy(step).start()

        return carry

    lax.fori_loop(0, steps, compute, 0)
    back[REMOTE] = result[REMOTE]
    total[...] = jnp.zeros_like(total)

    def combine(order, carry):
        step = (order + REMOTE) % steps

        @pl.when(step != REMOTE)
        def _():
            return_copy(step).wait_recv()

        total[...] += matmul_t(choice(step), back[step])
        return carry

    lax.fori_loop(0, steps, combine, 0)
    out_ref[...] = total[...].astype(out_ref.dtype)

    def drain(step, carry):
        dispatch_copy(step).wait_send()
        return_copy(step).wait_send()
        return carry

    lax.fori_loop(0, REMOTE, drain, 0)
    lax.fori_loop(REMOTE + 1, steps, drain, 0)


def packed_kernel(slot_count, tok_ref, ids_ref, slots_ref, gate_hbm, up_hbm, down_hbm, out_ref, full_ref,
                  gate_w, up_w, down_w, hidden, total,
                  own_hot, own_send, own_recv, own_result, own_back,
                  z_hot, z_send, z_recv, z_result, z_back,
                  list_hot, list_send, lists, codes_out, codes_in, shares, core_in, z_in, list_back,
                  flag_src, flags, group_src, group_in,
                  w_sem, own_sem, z_sem, list_sem, code_sem, share_sem, flag_sem):
    rows, width = tok_ref.shape
    node, expert = lax.axis_index("node"), lax.axis_index("expert")
    inner = (node + 1) // 2 == 1
    roles = ((INNER, inner), (OUTER, jnp.logical_not(inner)))
    loads = load_weights((gate_hbm, up_hbm, down_hbm), (gate_w, up_w, down_w), w_sem)

    barrier = pltpu.get_barrier_semaphore()
    twin = {"data": (lax.axis_index("data") + 1) % 2}
    pl.semaphore_signal(barrier, inc=1, device_id=twin, device_id_type=MESH)

    def greet(q, carry):
        pl.semaphore_signal(barrier, inc=1, device_id=place(q // 4, q % 4), device_id_type=MESH)
        return carry

    lax.fori_loop(1, 16, greet, 0)

    def own_copy(w):
        return remote(own_send.at[w], own_recv.at[w], own_sem.at[0, w], own_sem.at[1, w], place(0, w))

    def own_return(w):
        return remote(own_result.at[w], own_back.at[w], own_sem.at[2, w], own_sem.at[3, w], place(0, w))

    def z_part(k):
        return pl.ds(k * BASE, BASE) if k < 2 else pl.ds(2 * BASE, slot_count)

    def z_copy(w, k):
        return remote(z_send.at[w, z_part(k)], z_recv.at[w, z_part(k)], z_sem.at[0, 3 * w + k], z_sem.at[1, 3 * w + k],
                      place((2, 3, 1)[k], w))

    def z_return(w, k):
        return remote(z_result.at[w, z_part(k)], z_back.at[w, z_part(k)], z_sem.at[2, 3 * w + k], z_sem.at[3, 3 * w + k],
                      place((2, 3, 1)[k], w))

    sent = pl.ds(0, SPILL)
    kind = 1 - ((node + 1) // 2 + 1) % 2

    def list_copy(src, codes_src, at, go, device):
        w, i = at
        come = 2 * w + i
        named = pl.ds(0, 2)
        return Both(remote(src.at[sent], lists.at[w, i, sent], list_sem.at[go], list_sem.at[come], device),
                    remote(codes_src.at[named], codes_in.at[w, i, named], code_sem.at[go], code_sem.at[come], device))

    def list_out(h):
        return list_copy(list_send.at[h], codes_out.at[h], (2 * h, kind), 8 + h,
                         {"node": 2 - node // 2, "expert": flip(expert, 2 * h)})

    def arrived(w, i):
        return list_copy(lists.at[w, i], codes_in.at[w, i], (w, i), 8, place(0, 1))

    def forward_z(w, i):
        return list_copy(lists.at[w, i], codes_in.at[w, i], (w, 1 - i), 10 + w + i, place(1, 0))

    def forward_core(w, i):
        return list_copy(lists.at[w, i], codes_in.at[w, i], (w + 1, i), 14 + w + i, place(0, 1))

    def share_core(w, i):
        return remote(shares.at[w, i, sent], core_in.at[w // 2, i, sent], share_sem.at[2 * w + i],
                      share_sem.at[8 + 2 * (w // 2) + i], place(0, 1))

    def share_z(w, i):
        return remote(shares.at[w, i, sent], z_in.at[w // 2, 1 - i, sent], share_sem.at[2 * w + i],
                      share_sem.at[13 + w - i], place(1, 0))

    def share_home(w, i):
        return remote(shares.at[w, i, sent], list_back.at[w // 2, sent], share_sem.at[2 * w + i],
                      share_sem.at[16 + w // 2], place(2 + i, w))

    def flag_copy(q):
        return remote(flag_src.at[pl.ds(0, 1)], flags.at[q, pl.ds(0, 1)], flag_sem.at[0, q], flag_sem.at[1, q], place(q // 4, q % 4))

    def group_copy():
        return remote(group_src.at[pl.ds(0, 1)], group_in.at[pl.ds(0, 1)], flag_sem.at[0, 0], flag_sem.at[1, 0], twin)

    ids, slots = ids_ref[...], slots_ref[...]
    flat_pos = jnp.where(slots >= 0, ids * slot_count + slots, 16 * slot_count)
    far_spill = jnp.logical_and(ids // 8 != node // 2, slots >= BASE)
    lanes = 128
    folds = rows // lanes
    upto = one_hot(lax.broadcasted_iota(jnp.int32, (lanes, lanes), 0) <= lax.broadcasted_iota(jnp.int32, (lanes, lanes), 1))
    before = one_hot(lax.broadcasted_iota(jnp.int32, (folds, folds), 1) < lax.broadcasted_iota(jnp.int32, (folds, folds), 0))
    codes = jnp.concatenate([ids, slots] + [jnp.zeros_like(ids)] * (CODES - 2), axis=0).astype(jnp.float32).astype(jnp.bfloat16)
    excess = 0.0
    for h in range(2):
        column = (expert // 2 + h) % 2
        spills = jnp.logical_and(far_spill, ids // 2 % 2 == column).astype(jnp.float32)
        grid = jnp.concatenate([spills[:, i * lanes:(i + 1) * lanes] for i in range(folds)], axis=0)
        marks = grid.astype(jnp.bfloat16)
        order = matmul(marks, upto) + jnp.sum(matmul(before, marks), axis=1, keepdims=True)
        order = jnp.where(grid > 0, order, 0.0).astype(jnp.int32) - 1
        order = jnp.concatenate([order[i:i + 1, :] for i in range(folds)], axis=1)
        order = jnp.where(order < SPILL, order, -1)
        list_hot[h] = one_hot(order == lax.broadcasted_iota(jnp.int32, (PADDED, rows), 0))
        named = lax.dot_general(codes, list_hot[h], (((1,), (1,)), ((), ())), preferred_element_type=jnp.float32)
        list_send[h] = matmul(list_hot[h], tok_ref[...]).astype(jnp.bfloat16)
        codes_out[h] = named[0:8]
        list_back[h, SPILL:PADDED] = jnp.zeros((PADDED - SPILL, width), jnp.bfloat16)
        excess = jnp.maximum(excess, jnp.sum(spills) - SPILL)
    flag_src[...] = jnp.broadcast_to(excess, flag_src.shape)
    for w in range(4):
        for i in range(2):
            lists[w, i, SPILL:PADDED] = jnp.zeros((PADDED - SPILL, width), jnp.bfloat16)

    def target(by_node, w, count):
        return lax.broadcasted_iota(jnp.int32, (count, rows), 0) + expert_of(by_node, w) * slot_count

    def own_pick(w, carry):
        own_hot[w] = one_hot(flat_pos == target(0, w, slot_count))
        own_send[w] = matmul(own_hot[w], tok_ref[...]).astype(jnp.bfloat16)

        return carry

    lax.fori_loop(0, 4, own_pick, 0)
    pl.semaphore_wait(barrier, 16)
    list_out(0).start()
    list_out(1).start()
    for w in (2, 3, 1):
        own_copy(w).start()

    def flag_out(q, carry):
        flag_copy(q).start()
        return carry

    lax.fori_loop(1, 16, flag_out, 0)

    def z_pick(w, carry):
        z_hot[w, 0:BASE] = one_hot(flat_pos == target(2, w, BASE))
        z_hot[w, BASE:2 * BASE] = one_hot(flat_pos == target(3, w, BASE))
        z_hot[w, 2 * BASE:] = one_hot(flat_pos == target(1, w, slot_count))
        z_send[w] = matmul(z_hot[w], tok_ref[...]).astype(jnp.bfloat16)

        for role, is_role in roles:
            early = [v for v in range(4) if role["near"][v] == 0]
            if early == [0, 1, 2, 3]:
                @pl.when(is_role)
                def _():
                    z_copy(w, 2).start()

        return carry

    lax.fori_loop(0, 4, z_pick, 0)
    for load in loads:
        load.wait()

    def ffn(block):
        return expert_ffn(block, gate_w, up_w, down_w, hidden)

    own_recv[0] = own_send[0]

    def own_step(w, carry):
        @pl.when(w > 0)
        def _():
            own_copy(w).wait_recv()

        own_result[w] = ffn(own_recv[w])

        @pl.when(w > 0)
        def _():
            own_return(w).start()

        return carry


    me = node * 4 + expert
    over = slot_count - BASE

    near = slice(2 * BASE, 2 * BASE + slot_count)
    far = slice(0, 2 * BASE)

    def near_step(w, carry):
        z_copy(w, 2).wait_recv()
        z_result[w, near] = ffn(z_recv[w, near])
        return carry

    def far_step(w, carry):
        z_copy(w, 0).wait_recv()
        z_copy(w, 1).wait_recv()
        z_result[w, far] = ffn(z_recv[w, far])
        z_return(w, 0).start()
        z_return(w, 1).start()
        return carry

    def list_step(r, carry):
        w = r + 1 - 2 * (r % 2)

        @pl.when(r % 2 == 0)
        def _():
            @pl.when(jnp.logical_not(inner))
            def _():
                for i in range(2):
                    arrived(w - 1, i).wait_recv()
                    forward_core(w - 1, i).start()

            for i in range(2):
                arrived(w, i).wait_recv()

        mine, blocks = [], []
        for i in range(2):
            codes = codes_in[w, i]
            slot = lax.broadcasted_iota(jnp.int32, (over, PADDED), 0) + BASE
            hit = jnp.logical_and(codes[0:1].astype(jnp.int32) == me, codes[1:2].astype(jnp.int32) == slot)
            mine.append(one_hot(hit))
            blocks.append(matmul(mine[i], lists[w, i]).astype(jnp.bfloat16))
        y = ffn(jnp.concatenate(blocks, axis=0))
        for i in range(2):
            shares[w, i] = matmul_t(mine[i], y[i * over:(i + 1) * over]).astype(jnp.bfloat16)

        @pl.when(r % 2 == 0)
        def _():
            for i in range(2):
                share_core(w, i).start()

        @pl.when(r % 2 == 1)
        def _():
            for i in range(2):
                share_core(w + 1, i).wait_recv()
                shares[w, i, 0:SPILL] += core_in[w // 2, i, 0:SPILL]

                @pl.when(jnp.logical_not(inner))
                def _():
                    share_z(w, i).start()

        return carry

    def forward_list(w, i):
        arrived(w, i).wait_recv()
        forward_core(w, i).start()
        forward_z(w, i).start()

    def merge_home(w):
        for i in range(2):
            share_z(w, 1 - i).wait_recv()
            shares[w, i, 0:SPILL] += z_in[w // 2, i, 0:SPILL]
            share_home(w, i).start()

    def acts(role, slot):
        same = kind_of_far[role is INNER]
        found = []
        for w in range(4):
            if role["near"][w] == slot and role["near"] != (0, 0, 0, 0):
                found.append(z_copy(w, 2).start)
        for name, k in (("to_inner", same), ("to_outer", 1 - same)):
            found += [z_copy(w, k).start for w in range(4) if role[name][w] == slot]
        found += [z_return(w, 2).start for w in range(4) if role["near_back"][w] == slot]
        if role is INNER:
            found += [functools.partial(forward_list, w, i) for w, i, when in role["lists"] if when == slot]
            found += [functools.partial(merge_home, w) for w in (0, 2) if role["home"][w // 2] == slot]
        return found

    kind_of_far = {True: 1, False: 0}

    def fire(at):
        for role, is_role in roles:
            for slot in range(len(role["order"])):
                todo = acts(role, slot)
                if todo:
                    @pl.when(jnp.logical_and(at == slot, is_role))
                    def _():
                        for act in todo:
                            act()

    def table(values, at):
        inner_values, outer_values = values
        total = 0
        for slot, (a, b) in enumerate(zip(inner_values, outer_values)):
            total = total + jnp.where(at == slot, a if a == b else jnp.where(inner, a, b), 0)
        return total

    orders = [role["order"] for role, _ in roles]
    sorts = [[KINDS.index(letter) for letter in order] for order in orders]
    turns = [[order[:slot].count(letter) for slot, letter in enumerate(order)] for order in orders]

    def slot_step(at, carry):
        fire(at)
        sort, turn = table(sorts, at), table(turns, at)
        for number, step in enumerate((own_step, near_step, far_step, list_step)):
            @pl.when(sort == number)
            def _():
                step(turn, 0)

        return carry

    lax.fori_loop(0, 16, slot_step, 0)
    own_back[0] = own_result[0]
    for role, is_role in roles:
        todo = acts(role, 16)
        if todo:
            @pl.when(is_role)
            def _():
                for act in todo:
                    act()

    def flag_in(q, carry):
        flag_copy(q).wait_recv()
        return carry

    lax.fori_loop(1, 16, flag_in, 0)
    flags[0] = flag_src[...]
    group_src[0:1] = jnp.max(flags[:, 0:1], axis=0)

    flag_copy(1).wait_send()
    group_copy().start()

    for w in range(1, 4):
        own_return(w).wait_recv()
    total[...] = matmul_t(own_hot[...].reshape(4 * slot_count, rows), own_back[...].reshape(4 * slot_count, width))

    def z_combine(w, carry):
        for k in (2, 0, 1):
            z_return(w, k).wait_recv()
        total[...] += matmul_t(z_hot[w], z_back[w])
        return carry

    lax.fori_loop(0, 4, z_combine, 0)
    share_home(0, 0).wait_recv()
    total[...] += matmul_t(list_hot[0], list_back[0])
    share_home(2, 0).wait_recv()
    out_ref[...] = (total[...] + matmul_t(list_hot[1], list_back[1])).astype(out_ref.dtype)

    group_copy().wait_recv()
    full_ref[0, 0] = (jnp.max(jnp.maximum(group_src[0:1], group_in[0:1])) > 0.0).astype(jnp.int32)

    for w in range(1, 4):
        own_copy(w).wait_send()
        own_return(w).wait_send()
    for w in range(4):
        for k in range(3):
            z_copy(w, k).wait_send()
            z_return(w, k).wait_send()
    group_copy().wait_send()

    def flag_sent(q, carry):
        flag_copy(q).wait_send()
        return carry

    lax.fori_loop(2, 16, flag_sent, 0)
    for i in range(2):
        list_out(i).wait_send()
        for w in (0, 2):
            forward_core(w, i).wait_send()
            share_core(w + 1, i).wait_send()

            @pl.when(inner)
            def _():
                forward_z(w, i).wait_send()
                share_home(w, i).wait_send()

            @pl.when(jnp.logical_not(inner))
            def _():
                share_z(w, i).wait_send()


def solution(mesh):
    group_size = mesh.shape["node"] * mesh.shape["expert"]
    tok_spec = P(("data", "node", "expert"), None)
    weight_spec = P(("node", "expert"), None, None)

    def local_layer(tokens, expert_ids, gate_weights, slot_ids, w_gate, w_up, w_down):
        rows, width = tokens.shape
        ff = w_gate.shape[2]
        slot_count = capacity(rows, 1, group_size)
        vmem = pl.BlockSpec(memory_space=pltpu.VMEM)
        smem = pl.BlockSpec(memory_space=pltpu.SMEM)
        hbm = pl.BlockSpec(memory_space=pl.ANY)
        dma = pltpu.SemaphoreType.DMA
        weights = [pltpu.VMEM((width, ff), jnp.bfloat16), pltpu.VMEM((width, ff), jnp.bfloat16),
                   pltpu.VMEM((ff, width), jnp.bfloat16)]
        hidden = pltpu.VMEM((2 * (slot_count - BASE), ff), jnp.bfloat16)
        total = pltpu.VMEM((rows, width), jnp.float32)
        picked_shape = jax.ShapeDtypeStruct((rows, width), jnp.bfloat16)
        operands = (tokens, expert_ids.reshape(1, rows), slot_ids.reshape(1, rows), w_gate, w_up, w_down)

        def bf16(*shape):
            return pltpu.VMEM(shape, jnp.bfloat16)

        def params(number):
            return pltpu.CompilerParams(collective_id=number, has_side_effects=True, vmem_limit_bytes=60 * 1024 * 1024)

        def scaled(picked):
            return (gate_weights * picked.astype(jnp.float32)).astype(jnp.bfloat16)

        def padded():
            block = (group_size, slot_count, width)
            return pl.pallas_call(
                functools.partial(padded_kernel, slot_count), out_shape=picked_shape,
                in_specs=[vmem] * 3 + [hbm] * 3, out_specs=vmem,
                scratch_shapes=weights + [bf16(*block)] * 4 + [hidden, total, dma((3,))] + [dma((group_size,))] * 4,
                compiler_params=params(1), name="padded_layer",
            )(*operands)

        own = (4, slot_count, width)
        zed = (4, 2 * BASE + slot_count, width)
        flag = pltpu.VMEM((8, 128), jnp.float32)
        picked, full = pl.pallas_call(
            functools.partial(packed_kernel, slot_count),
            out_shape=(picked_shape, jax.ShapeDtypeStruct((1, 1), jnp.int32)),
            in_specs=[vmem] * 3 + [hbm] * 3, out_specs=(vmem, smem),
            scratch_shapes=weights + [hidden, total]
            + [bf16(4, slot_count, rows)] + [bf16(*own)] * 4
            + [bf16(4, 2 * BASE + slot_count, rows)] + [bf16(*zed)] * 4
            + [bf16(2, PADDED, rows), bf16(2, PADDED, width), bf16(4, 2, PADDED, width),
               pltpu.VMEM((2, 8, PADDED), jnp.float32), pltpu.VMEM((4, 2, 8, PADDED), jnp.float32), bf16(4, 2, PADDED, width),
               bf16(2, 2, PADDED, width), bf16(2, 2, PADDED, width), bf16(2, PADDED, width)]
            + [flag, pltpu.VMEM((16, 8, 128), jnp.float32), flag, flag]
            + [dma((3,)), dma((4, 4)), dma((4, 12)), dma((18,)), dma((18,)), dma((18,)), dma((2, 16))],
            compiler_params=params(0), name="packed_layer",
        )(*operands)
        return lax.cond(full[0, 0] > 0, lambda: scaled(padded()), lambda: scaled(picked))

    return jax.shard_map(local_layer, mesh=mesh, in_specs=(tok_spec,) * 4 + (weight_spec,) * 3,
                         out_specs=tok_spec, check_vma=False)
```

```python
import functools

import jax
import jax.numpy as jnp
from jax import lax
from jax.experimental import pallas as pl
from jax.experimental.pallas import tpu as pltpu
from jax.sharding import PartitionSpec as P

CAP_FACTOR = 2
MESH = pl.DeviceIdType.MESH
FF_TILE = 512
REMOTE = 12
BASE = 48
SPILL = 160
PADDED = 256
CODES = 16
INNER = dict(order="oollolloffffnnnn", near=(0, 0, 0, 0), to_inner=(5, 5, 6, 6), to_outer=(6, 6, 7, 7),
             near_back=(14, 15, 16, 16), home=(13, 16), lists=((0, 0, 2), (2, 0, 2), (0, 1, 5), (2, 1, 5)))
OUTER = dict(order="oooonnnnllllffff", near=(0, 0, 0, 0), to_inner=(4, 4, 4, 4), to_outer=(8, 8, 8, 8),
             near_back=(10, 10, 13, 13))
KINDS = "onfl"


def capacity(rows, top_k, experts):
    return ((CAP_FACTOR * rows * top_k + 8 * experts - 1) // (8 * experts)) * 8


def flip(value, by):
    return 2 * ((value // 2 + by // 2) % 2) + (value + by) % 2


def place(by_node, by_expert):
    return {"node": flip(lax.axis_index("node"), by_node), "expert": flip(lax.axis_index("expert"), by_expert)}


def expert_of(by_node, by_expert):
    at = place(by_node, by_expert)
    return at["node"] * 4 + at["expert"]


def one_hot(mask):
    return mask.astype(jnp.float32).astype(jnp.bfloat16)


def matmul(a, b):
    return jnp.dot(a, b, preferred_element_type=jnp.float32)


def matmul_t(a, b):
    return lax.dot_general(a, b, (((0,), (0,)), ((), ())), preferred_element_type=jnp.float32)


def expert_ffn(block, gate_w, up_w, down_w, hidden):
    count = block.shape[0]
    for start in range(0, hidden.shape[1], FF_TILE):
        cols = slice(start, start + FF_TILE)
        gate = matmul(block, gate_w[:, cols])
        up = matmul(block, up_w[:, cols])
        hidden[0:count, cols] = (jax.nn.silu(gate) * up).astype(jnp.bfloat16)
    return matmul(hidden[0:count], down_w[...]).astype(jnp.bfloat16)


def load_weights(refs, scratch, sems):
    loads = [pltpu.make_async_copy(src.at[0], dst, sems.at[i]) for i, (src, dst) in enumerate(zip(refs, scratch))]
    for load in loads:
        load.start()
    return loads


def remote(src, dst, go, come, device):
    return pltpu.make_async_remote_copy(
        src_ref=src, dst_ref=dst, send_sem=go, recv_sem=come, device_id=device, device_id_type=MESH)


class Both:
    def __init__(self, first, second):
        self.copies = (first, second)

    def start(self):
        for copy in self.copies:
            copy.start()

    def wait_send(self):
        for copy in self.copies:
            copy.wait_send()

    def wait_recv(self):
        for copy in self.copies:
            copy.wait_recv()


def padded_kernel(slot_count, tok_ref, ids_ref, slots_ref, gate_hbm, up_hbm, down_hbm, out_ref,
                  gate_w, up_w, down_w, send, recv, result, back, hidden, total,
                  w_sem, go_sem, come_sem, ret_go_sem, ret_come_sem):
    rows, width = tok_ref.shape
    steps = 16
    loads = load_weights((gate_hbm, up_hbm, down_hbm), (gate_w, up_w, down_w), w_sem)
    barrier = pltpu.get_barrier_semaphore()

    def relative(step):
        far = 1 - step // REMOTE
        return far * (1 + (step % 3 + 1) % 3), far * (step // 3) + (1 - far) * (step - REMOTE)

    def greet(step, carry):
        pl.semaphore_signal(barrier, inc=1, device_id=place(*relative(step)), device_id_type=MESH)
        return carry

    lax.fori_loop(0, REMOTE, greet, 0)
    lax.fori_loop(REMOTE + 1, steps, greet, 0)

    def dispatch_copy(step):
        return remote(send.at[step], recv.at[step], go_sem.at[step], come_sem.at[step], place(*relative(step)))

    def return_copy(step):
        return remote(result.at[step], back.at[step], ret_go_sem.at[step], ret_come_sem.at[step], place(*relative(step)))

    flat_pos = jnp.where(slots_ref[...] >= 0, ids_ref[...] * slot_count + slots_ref[...], steps * slot_count)

    def choice(step):
        first = expert_of(*relative(step)) * slot_count
        return one_hot(flat_pos == lax.broadcasted_iota(jnp.int32, (slot_count, rows), 0) + first)

    def pick(step):
        return matmul(choice(step), tok_ref[...]).astype(jnp.bfloat16)

    pl.semaphore_wait(barrier, steps - 1)

    def dispatch(step, carry):
        send[step] = pick(step)
        dispatch_copy(step).start()
        return carry

    lax.fori_loop(0, REMOTE, dispatch, 0)
    lax.fori_loop(REMOTE + 1, steps, dispatch, 0)
    recv[REMOTE] = pick(REMOTE)
    for load in loads:
        load.wait()

    def compute(order, carry):
        step = (order + REMOTE) % steps

        @pl.when(step != REMOTE)
        def _():
            dispatch_copy(step).wait_recv()

        result[step] = expert_ffn(recv[step], gate_w, up_w, down_w, hidden)

        @pl.when(step != REMOTE)
        def _():
            return_copy(step).start()

        return carry

    lax.fori_loop(0, steps, compute, 0)
    back[REMOTE] = result[REMOTE]
    total[...] = jnp.zeros_like(total)

    def combine(order, carry):
        step = (order + REMOTE) % steps

        @pl.when(step != REMOTE)
        def _():
            return_copy(step).wait_recv()

        total[...] += matmul_t(choice(step), back[step])
        return carry

    lax.fori_loop(0, steps, combine, 0)
    out_ref[...] = total[...].astype(out_ref.dtype)

    def drain(step, carry):
        dispatch_copy(step).wait_send()
        return_copy(step).wait_send()
        return carry

    lax.fori_loop(0, REMOTE, drain, 0)
    lax.fori_loop(REMOTE + 1, steps, drain, 0)


def packed_kernel(slot_count, tok_ref, ids_ref, slots_ref, gate_hbm, up_hbm, down_hbm, out_ref, full_ref,
                  gate_w, up_w, down_w, hidden, total,
                  own_hot, own_send, own_recv, own_result, own_back,
                  z_hot, z_send, z_recv, z_result, z_back,
                  list_hot, list_send, lists, codes_out, codes_in, shares, core_in, z_in, list_back,
                  flag_src, flags, group_src, group_in,
                  w_sem, own_sem, z_sem, list_sem, code_sem, share_sem, flag_sem):
    rows, width = tok_ref.shape
    node, expert = lax.axis_index("node"), lax.axis_index("expert")
    inner = (node + 1) // 2 == 1
    roles = ((INNER, inner), (OUTER, jnp.logical_not(inner)))
    barrier = pltpu.get_barrier_semaphore()
    twin = {"data": (lax.axis_index("data") + 1) % 2}
    pl.semaphore_signal(barrier, inc=1, device_id=twin, device_id_type=MESH)

    def greet(q, carry):
        pl.semaphore_signal(barrier, inc=1, device_id=place(q // 4, q % 4), device_id_type=MESH)
        return carry

    lax.fori_loop(1, 16, greet, 0)
    loads = load_weights((gate_hbm, up_hbm, down_hbm), (gate_w, up_w, down_w), w_sem)

    def own_copy(w):
        return remote(own_send.at[w], own_recv.at[w], own_sem.at[0, w], own_sem.at[1, w], place(0, w))

    def own_return(w):
        return remote(own_result.at[w], own_back.at[w], own_sem.at[2, w], own_sem.at[3, w], place(0, w))

    def z_part(k):
        return pl.ds(k * BASE, BASE) if k < 2 else pl.ds(2 * BASE, slot_count)

    def z_copy(w, k):
        return remote(z_send.at[w, z_part(k)], z_recv.at[w, z_part(k)], z_sem.at[0, 3 * w + k], z_sem.at[1, 3 * w + k],
                      place((2, 3, 1)[k], w))

    def z_return(w, k):
        return remote(z_result.at[w, z_part(k)], z_back.at[w, z_part(k)], z_sem.at[2, 3 * w + k], z_sem.at[3, 3 * w + k],
                      place((2, 3, 1)[k], w))

    sent = pl.ds(0, SPILL)
    kind = 1 - ((node + 1) // 2 + 1) % 2

    def list_copy(src, codes_src, at, go, device):
        w, i = at
        come = 2 * w + i
        named = pl.ds(0, 2)
        return Both(remote(src.at[sent], lists.at[w, i, sent], list_sem.at[go], list_sem.at[come], device),
                    remote(codes_src.at[named], codes_in.at[w, i, named], code_sem.at[go], code_sem.at[come], device))

    def list_out(h):
        return list_copy(list_send.at[h], codes_out.at[h], (2 * h, kind), 8 + h,
                         {"node": 2 - node // 2, "expert": flip(expert, 2 * h)})

    def arrived(w, i):
        return list_copy(lists.at[w, i], codes_in.at[w, i], (w, i), 8, place(0, 1))

    def forward_z(w, i):
        return list_copy(lists.at[w, i], codes_in.at[w, i], (w, 1 - i), 10 + w + i, place(1, 0))

    def forward_core(w, i):
        return list_copy(lists.at[w, i], codes_in.at[w, i], (w + 1, i), 14 + w + i, place(0, 1))

    def share_core(w, i):
        return remote(shares.at[w, i, sent], core_in.at[w // 2, i, sent], share_sem.at[2 * w + i],
                      share_sem.at[8 + 2 * (w // 2) + i], place(0, 1))

    def share_z(w, i):
        return remote(shares.at[w, i, sent], z_in.at[w // 2, 1 - i, sent], share_sem.at[2 * w + i],
                      share_sem.at[13 + w - i], place(1, 0))

    def share_home(w, i):
        return remote(shares.at[w, i, sent], list_back.at[w // 2, sent], share_sem.at[2 * w + i],
                      share_sem.at[16 + w // 2], place(2 + i, w))

    def flag_copy(q):
        return remote(flag_src.at[pl.ds(0, 1)], flags.at[q, pl.ds(0, 1)], flag_sem.at[0, q], flag_sem.at[1, q], place(q // 4, q % 4))

    def group_copy():
        return remote(group_src.at[pl.ds(0, 1)], group_in.at[pl.ds(0, 1)], flag_sem.at[0, 0], flag_sem.at[1, 0], twin)

    ids, slots = ids_ref[...], slots_ref[...]
    flat_pos = jnp.where(slots >= 0, ids * slot_count + slots, 16 * slot_count)
    far_spill = jnp.logical_and(ids // 8 != node // 2, slots >= BASE)
    lanes = 128
    folds = rows // lanes
    upto = one_hot(lax.broadcasted_iota(jnp.int32, (lanes, lanes), 0) <= lax.broadcasted_iota(jnp.int32, (lanes, lanes), 1))
    before = one_hot(lax.broadcasted_iota(jnp.int32, (folds, folds), 1) < lax.broadcasted_iota(jnp.int32, (folds, folds), 0))
    codes = jnp.concatenate([ids, slots] + [jnp.zeros_like(ids)] * (CODES - 2), axis=0).astype(jnp.float32).astype(jnp.bfloat16)
    excess = 0.0
    for h in range(2):
        column = (expert // 2 + h) % 2
        spills = jnp.logical_and(far_spill, ids // 2 % 2 == column).astype(jnp.float32)
        grid = jnp.concatenate([spills[:, i * lanes:(i + 1) * lanes] for i in range(folds)], axis=0)
        marks = grid.astype(jnp.bfloat16)
        order = matmul(marks, upto) + jnp.sum(matmul(before, marks), axis=1, keepdims=True)
        order = jnp.where(grid > 0, order, 0.0).astype(jnp.int32) - 1
        order = jnp.concatenate([order[i:i + 1, :] for i in range(folds)], axis=1)
        order = jnp.where(order < SPILL, order, -1)
        list_hot[h] = one_hot(order == lax.broadcasted_iota(jnp.int32, (PADDED, rows), 0))
        named = lax.dot_general(codes, list_hot[h], (((1,), (1,)), ((), ())), preferred_element_type=jnp.float32)
        list_send[h, 0:SPILL] = matmul(list_hot[h, 0:SPILL], tok_ref[...]).astype(jnp.bfloat16)
        codes_out[h] = named[0:8]
        list_back[h, SPILL:PADDED] = jnp.zeros((PADDED - SPILL, width), jnp.bfloat16)
        excess = jnp.maximum(excess, jnp.sum(spills) - SPILL)
    flag_src[...] = jnp.broadcast_to(excess, flag_src.shape)

    def target(by_node, w, count):
        return lax.broadcasted_iota(jnp.int32, (count, rows), 0) + expert_of(by_node, w) * slot_count

    def own_pick(w, carry):
        own_hot[w] = one_hot(flat_pos == target(0, w, slot_count))
        own_send[w] = matmul(own_hot[w], tok_ref[...]).astype(jnp.bfloat16)

        return carry

    lax.fori_loop(0, 4, own_pick, 0)
    pl.semaphore_wait(barrier, 16)
    list_out(0).start()
    list_out(1).start()
    for w in (2, 3, 1):
        own_copy(w).start()

    def flag_out(q, carry):
        flag_copy(q).start()
        return carry

    lax.fori_loop(1, 16, flag_out, 0)

    def z_pick(w, carry):
        z_hot[w, 0:BASE] = one_hot(flat_pos == target(2, w, BASE))
        z_hot[w, BASE:2 * BASE] = one_hot(flat_pos == target(3, w, BASE))
        z_hot[w, 2 * BASE:] = one_hot(flat_pos == target(1, w, slot_count))
        z_send[w] = matmul(z_hot[w], tok_ref[...]).astype(jnp.bfloat16)

        for role, is_role in roles:
            early = [v for v in range(4) if role["near"][v] == 0]
            if early == [0, 1, 2, 3]:
                @pl.when(is_role)
                def _():
                    z_copy(w, 2).start()

        return carry

    lax.fori_loop(0, 4, z_pick, 0)
    for w in range(4):
        for i in range(2):
            lists[w, i, SPILL:PADDED] = jnp.zeros((PADDED - SPILL, width), jnp.bfloat16)
    for load in loads:
        load.wait()

    def ffn(block):
        return expert_ffn(block, gate_w, up_w, down_w, hidden)

    own_recv[0] = own_send[0]

    def own_step(w, carry):
        @pl.when(w > 0)
        def _():
            own_copy(w).wait_recv()

        own_result[w] = ffn(own_recv[w])

        @pl.when(w > 0)
        def _():
            own_return(w).start()

        return carry


    me = node * 4 + expert
    over = slot_count - BASE

    near = slice(2 * BASE, 2 * BASE + slot_count)
    far = slice(0, 2 * BASE)

    def near_step(w, carry):
        z_copy(w, 2).wait_recv()
        z_result[w, near] = ffn(z_recv[w, near])
        return carry

    def far_step(w, carry):
        z_copy(w, 0).wait_recv()
        z_copy(w, 1).wait_recv()
        z_result[w, far] = ffn(z_recv[w, far])
        z_return(w, 0).start()
        z_return(w, 1).start()
        return carry

    def list_step(r, carry):
        i = 1 - kind + (r // 2) * (2 * kind - 1)
        odd = 1 - r % 2

        @pl.when(odd == 1)
        def _():
            @pl.when(jnp.logical_not(inner))
            def _():
                for w in (0, 2):
                    arrived(w, i).wait_recv()
                    forward_core(w, i).start()

            for w in (1, 3):
                arrived(w, i).wait_recv()

        mine, blocks = [], []
        for h in range(2):
            w = 2 * h + odd
            codes = codes_in[w, i]
            slot = lax.broadcasted_iota(jnp.int32, (over, PADDED), 0) + BASE
            hit = jnp.logical_and(codes[0:1].astype(jnp.int32) == me, codes[1:2].astype(jnp.int32) == slot)
            mine.append(one_hot(hit))
            blocks.append(matmul(mine[h], lists[w, i]).astype(jnp.bfloat16))
        y = ffn(jnp.concatenate(blocks, axis=0))
        for h in range(2):
            shares[2 * h + odd, i] = matmul_t(mine[h], y[h * over:(h + 1) * over]).astype(jnp.bfloat16)

        @pl.when(odd == 1)
        def _():
            for w in (1, 3):
                share_core(w, i).start()

        @pl.when(odd == 0)
        def _():
            for w in (0, 2):
                share_core(w + 1, i).wait_recv()
                shares[w, i, 0:SPILL] += core_in[w // 2, i, 0:SPILL]

                @pl.when(jnp.logical_not(inner))
                def _():
                    share_z(w, i).start()

        return carry

    def forward_list(w, i):
        arrived(w, i).wait_recv()
        forward_core(w, i).start()
        forward_z(w, i).start()

    def merge_home(i):
        for w in (0, 2):
            share_z(w, 1 - i).wait_recv()
            shares[w, i, 0:SPILL] += z_in[w // 2, i, 0:SPILL]
            share_home(w, i).start()

    def acts(role, slot):
        same = kind_of_far[role is INNER]
        found = []
        for w in range(4):
            if role["near"][w] == slot and role["near"] != (0, 0, 0, 0):
                found.append(z_copy(w, 2).start)
        for name, k in (("to_inner", same), ("to_outer", 1 - same)):
            found += [z_copy(w, k).start for w in range(4) if role[name][w] == slot]
        found += [z_return(w, 2).start for w in range(4) if role["near_back"][w] == slot]
        if role is INNER:
            found += [functools.partial(forward_list, w, i) for w, i, when in role["lists"] if when == slot]
            found += [functools.partial(merge_home, i) for i in (0, 1) if role["home"][i] == slot]
        return found

    kind_of_far = {True: 1, False: 0}

    def fire(at):
        for role, is_role in roles:
            for slot in range(len(role["order"])):
                todo = acts(role, slot)
                if todo:
                    @pl.when(jnp.logical_and(at == slot, is_role))
                    def _():
                        for act in todo:
                            act()

    def table(values, at):
        inner_values, outer_values = values
        total = 0
        for slot, (a, b) in enumerate(zip(inner_values, outer_values)):
            total = total + jnp.where(at == slot, a if a == b else jnp.where(inner, a, b), 0)
        return total

    orders = [role["order"] for role, _ in roles]
    sorts = [[KINDS.index(letter) for letter in order] for order in orders]
    turns = [[order[:slot].count(letter) for slot, letter in enumerate(order)] for order in orders]

    def slot_step(at, carry):
        fire(at)
        sort, turn = table(sorts, at), table(turns, at)
        for number, step in enumerate((own_step, near_step, far_step, list_step)):
            @pl.when(sort == number)
            def _():
                step(turn, 0)

        return carry

    lax.fori_loop(0, 16, slot_step, 0)
    own_back[0] = own_result[0]
    for role, is_role in roles:
        todo = acts(role, 16)
        if todo:
            @pl.when(is_role)
            def _():
                for act in todo:
                    act()

    def flag_in(q, carry):
        flag_copy(q).wait_recv()
        return carry

    lax.fori_loop(1, 16, flag_in, 0)
    flags[0] = flag_src[...]
    group_src[0:1] = jnp.max(flags[:, 0:1], axis=0)

    flag_copy(1).wait_send()
    group_copy().start()

    for w in range(1, 4):
        own_return(w).wait_recv()
    total[...] = matmul_t(own_hot[...].reshape(4 * slot_count, rows), own_back[...].reshape(4 * slot_count, width))

    def z_combine(w, carry):
        for k in (2, 0, 1):
            z_return(w, k).wait_recv()
        total[...] += matmul_t(z_hot[w], z_back[w])
        return carry

    lax.fori_loop(0, 4, z_combine, 0)
    group_copy().wait_recv()
    full_ref[0, 0] = (jnp.max(jnp.maximum(group_src[0:1], group_in[0:1])) > 0.0).astype(jnp.int32)

    for w in range(1, 4):
        own_copy(w).wait_send()
        own_return(w).wait_send()
    for w in range(4):
        for k in range(3):
            z_copy(w, k).wait_send()
            z_return(w, k).wait_send()
    group_copy().wait_send()

    def flag_sent(q, carry):
        flag_copy(q).wait_send()
        return carry

    lax.fori_loop(2, 16, flag_sent, 0)
    for i in range(2):
        list_out(i).wait_send()
        for w in (0, 2):
            forward_core(w, i).wait_send()
            share_core(w + 1, i).wait_send()

            @pl.when(inner)
            def _():
                forward_z(w, i).wait_send()
                share_home(w, i).wait_send()

            @pl.when(jnp.logical_not(inner))
            def _():
                share_z(w, i).wait_send()

    share_home(0, 0).wait_recv()
    total[...] += matmul_t(list_hot[0], list_back[0])
    share_home(2, 0).wait_recv()
    out_ref[...] = (total[...] + matmul_t(list_hot[1], list_back[1])).astype(out_ref.dtype)


def solution(mesh):
    group_size = mesh.shape["node"] * mesh.shape["expert"]
    tok_spec = P(("data", "node", "expert"), None)
    weight_spec = P(("node", "expert"), None, None)

    def local_layer(tokens, expert_ids, gate_weights, slot_ids, w_gate, w_up, w_down):
        rows, width = tokens.shape
        ff = w_gate.shape[2]
        slot_count = capacity(rows, 1, group_size)
        vmem = pl.BlockSpec(memory_space=pltpu.VMEM)
        smem = pl.BlockSpec(memory_space=pltpu.SMEM)
        hbm = pl.BlockSpec(memory_space=pl.ANY)
        dma = pltpu.SemaphoreType.DMA
        weights = [pltpu.VMEM((width, ff), jnp.bfloat16), pltpu.VMEM((width, ff), jnp.bfloat16),
                   pltpu.VMEM((ff, width), jnp.bfloat16)]
        hidden = pltpu.VMEM((2 * (slot_count - BASE), ff), jnp.bfloat16)
        total = pltpu.VMEM((rows, width), jnp.float32)
        picked_shape = jax.ShapeDtypeStruct((rows, width), jnp.bfloat16)
        operands = (tokens, expert_ids.reshape(1, rows), slot_ids.reshape(1, rows), w_gate, w_up, w_down)

        def bf16(*shape):
            return pltpu.VMEM(shape, jnp.bfloat16)

        def params(number):
            return pltpu.CompilerParams(collective_id=number, has_side_effects=True, vmem_limit_bytes=60 * 1024 * 1024)

        def scaled(picked):
            return (gate_weights * picked.astype(jnp.float32)).astype(jnp.bfloat16)

        def padded():
            block = (group_size, slot_count, width)
            return pl.pallas_call(
                functools.partial(padded_kernel, slot_count), out_shape=picked_shape,
                in_specs=[vmem] * 3 + [hbm] * 3, out_specs=vmem,
                scratch_shapes=weights + [bf16(*block)] * 4 + [hidden, total, dma((3,))] + [dma((group_size,))] * 4,
                compiler_params=params(1), name="padded_layer",
            )(*operands)

        own = (4, slot_count, width)
        zed = (4, 2 * BASE + slot_count, width)
        flag = pltpu.VMEM((8, 128), jnp.float32)
        picked, full = pl.pallas_call(
            functools.partial(packed_kernel, slot_count),
            out_shape=(picked_shape, jax.ShapeDtypeStruct((1, 1), jnp.int32)),
            in_specs=[vmem] * 3 + [hbm] * 3, out_specs=(vmem, smem),
            scratch_shapes=weights + [hidden, total]
            + [bf16(4, slot_count, rows)] + [bf16(*own)] * 4
            + [bf16(4, 2 * BASE + slot_count, rows)] + [bf16(*zed)] * 4
            + [bf16(2, PADDED, rows), bf16(2, PADDED, width), bf16(4, 2, PADDED, width),
               pltpu.VMEM((2, 8, PADDED), jnp.float32), pltpu.VMEM((4, 2, 8, PADDED), jnp.float32), bf16(4, 2, PADDED, width),
               bf16(2, 2, PADDED, width), bf16(2, 2, PADDED, width), bf16(2, PADDED, width)]
            + [flag, pltpu.VMEM((16, 8, 128), jnp.float32), flag, flag]
            + [dma((3,)), dma((4, 4)), dma((4, 12)), dma((18,)), dma((18,)), dma((18,)), dma((2, 16))],
            compiler_params=params(0), name="packed_layer",
        )(*operands)
        return lax.cond(full[0, 0] > 0, lambda: scaled(padded()), lambda: scaled(picked))

    return jax.shard_map(local_layer, mesh=mesh, in_specs=(tok_spec,) * 4 + (weight_spec,) * 3,
                         out_specs=tok_spec, check_vma=False)
```

```python
import functools

import jax
import jax.numpy as jnp
from jax import lax
from jax.experimental import pallas as pl
from jax.experimental.pallas import tpu as pltpu
from jax.sharding import PartitionSpec as P

CAP_FACTOR = 2
MESH = pl.DeviceIdType.MESH
FF_TILE = 512
REMOTE = 12
BASE = 48
SPILL = 160
PADDED = 256
CODES = 16
INNER = dict(order="oollolloffffnnnn", near=(0, 0, 0, 0), to_inner=(5, 5, 6, 6), to_outer=(6, 6, 7, 7),
             near_back=(14, 15, 16, 16), home=(13, 16), lists=((0, 0, 2), (2, 0, 2), (0, 1, 5), (2, 1, 5)))
OUTER = dict(order="oooonnnnllllffff", near=(0, 0, 0, 0), to_inner=(4, 4, 4, 4), to_outer=(8, 8, 8, 8),
             near_back=(10, 11, 12, 13))
KINDS = "onfl"


def capacity(rows, top_k, experts):
    return ((CAP_FACTOR * rows * top_k + 8 * experts - 1) // (8 * experts)) * 8


def flip(value, by):
    return 2 * ((value // 2 + by // 2) % 2) + (value + by) % 2


def place(by_node, by_expert):
    return {"node": flip(lax.axis_index("node"), by_node), "expert": flip(lax.axis_index("expert"), by_expert)}


def expert_of(by_node, by_expert):
    at = place(by_node, by_expert)
    return at["node"] * 4 + at["expert"]


def one_hot(mask):
    return mask.astype(jnp.float32).astype(jnp.bfloat16)


def matmul(a, b):
    return jnp.dot(a, b, preferred_element_type=jnp.float32)


def matmul_t(a, b):
    return lax.dot_general(a, b, (((0,), (0,)), ((), ())), preferred_element_type=jnp.float32)


def expert_ffn(block, gate_w, up_w, down_w, hidden):
    count = block.shape[0]
    for start in range(0, hidden.shape[1], FF_TILE):
        cols = slice(start, start + FF_TILE)
        gate = matmul(block, gate_w[:, cols])
        up = matmul(block, up_w[:, cols])
        hidden[0:count, cols] = (jax.nn.silu(gate) * up).astype(jnp.bfloat16)
    return matmul(hidden[0:count], down_w[...]).astype(jnp.bfloat16)


def load_weights(refs, scratch, sems):
    loads = [pltpu.make_async_copy(src.at[0], dst, sems.at[i]) for i, (src, dst) in enumerate(zip(refs, scratch))]
    for load in loads:
        load.start()
    return loads


def remote(src, dst, go, come, device):
    return pltpu.make_async_remote_copy(
        src_ref=src, dst_ref=dst, send_sem=go, recv_sem=come, device_id=device, device_id_type=MESH)


class Both:
    def __init__(self, first, second):
        self.copies = (first, second)

    def start(self):
        for copy in self.copies:
            copy.start()

    def wait_send(self):
        for copy in self.copies:
            copy.wait_send()

    def wait_recv(self):
        for copy in self.copies:
            copy.wait_recv()


def padded_kernel(slot_count, tok_ref, ids_ref, slots_ref, gate_hbm, up_hbm, down_hbm, out_ref,
                  gate_w, up_w, down_w, send, recv, result, back, hidden, total,
                  w_sem, go_sem, come_sem, ret_go_sem, ret_come_sem):
    rows, width = tok_ref.shape
    steps = 16
    loads = load_weights((gate_hbm, up_hbm, down_hbm), (gate_w, up_w, down_w), w_sem)
    barrier = pltpu.get_barrier_semaphore()

    def relative(step):
        far = 1 - step // REMOTE
        return far * (1 + (step % 3 + 1) % 3), far * (step // 3) + (1 - far) * (step - REMOTE)

    def greet(step, carry):
        pl.semaphore_signal(barrier, inc=1, device_id=place(*relative(step)), device_id_type=MESH)
        return carry

    lax.fori_loop(0, REMOTE, greet, 0)
    lax.fori_loop(REMOTE + 1, steps, greet, 0)

    def dispatch_copy(step):
        return remote(send.at[step], recv.at[step], go_sem.at[step], come_sem.at[step], place(*relative(step)))

    def return_copy(step):
        return remote(result.at[step], back.at[step], ret_go_sem.at[step], ret_come_sem.at[step], place(*relative(step)))

    flat_pos = jnp.where(slots_ref[...] >= 0, ids_ref[...] * slot_count + slots_ref[...], steps * slot_count)

    def choice(step):
        first = expert_of(*relative(step)) * slot_count
        return one_hot(flat_pos == lax.broadcasted_iota(jnp.int32, (slot_count, rows), 0) + first)

    def pick(step):
        return matmul(choice(step), tok_ref[...]).astype(jnp.bfloat16)

    pl.semaphore_wait(barrier, steps - 1)

    def dispatch(step, carry):
        send[step] = pick(step)
        dispatch_copy(step).start()
        return carry

    lax.fori_loop(0, REMOTE, dispatch, 0)
    lax.fori_loop(REMOTE + 1, steps, dispatch, 0)
    recv[REMOTE] = pick(REMOTE)
    for load in loads:
        load.wait()

    def compute(order, carry):
        step = (order + REMOTE) % steps

        @pl.when(step != REMOTE)
        def _():
            dispatch_copy(step).wait_recv()

        result[step] = expert_ffn(recv[step], gate_w, up_w, down_w, hidden)

        @pl.when(step != REMOTE)
        def _():
            return_copy(step).start()

        return carry

    lax.fori_loop(0, steps, compute, 0)
    back[REMOTE] = result[REMOTE]
    total[...] = jnp.zeros_like(total)

    def combine(order, carry):
        step = (order + REMOTE) % steps

        @pl.when(step != REMOTE)
        def _():
            return_copy(step).wait_recv()

        total[...] += matmul_t(choice(step), back[step])
        return carry

    lax.fori_loop(0, steps, combine, 0)
    out_ref[...] = total[...].astype(out_ref.dtype)

    def drain(step, carry):
        dispatch_copy(step).wait_send()
        return_copy(step).wait_send()
        return carry

    lax.fori_loop(0, REMOTE, drain, 0)
    lax.fori_loop(REMOTE + 1, steps, drain, 0)


def packed_kernel(slot_count, tok_hbm, ids_ref, slots_ref, gate_hbm, up_hbm, down_hbm, out_ref, full_ref,
                  tok_ref, gate_w, up_w, down_w, hidden, total,
                  own_hot, own_send, own_recv, own_result, own_back,
                  z_hot, z_send, z_recv, z_result, z_back,
                  list_hot, list_send, lists, codes_out, codes_in, shares, core_in, z_in, list_back,
                  flag_src, flags, group_src, group_in,
                  w_sem, own_sem, z_sem, list_sem, code_sem, share_sem, flag_sem):
    rows, width = tok_ref.shape
    node, expert = lax.axis_index("node"), lax.axis_index("expert")
    inner = (node + 1) // 2 == 1
    roles = ((INNER, inner), (OUTER, jnp.logical_not(inner)))
    barrier = pltpu.get_barrier_semaphore()
    twin = {"data": (lax.axis_index("data") + 1) % 2}
    pl.semaphore_signal(barrier, inc=1, device_id=twin, device_id_type=MESH)

    def greet(q, carry):
        pl.semaphore_signal(barrier, inc=1, device_id=place(q // 4, q % 4), device_id_type=MESH)
        return carry

    lax.fori_loop(1, 16, greet, 0)
    tok_load = pltpu.make_async_copy(tok_hbm, tok_ref, w_sem.at[3])
    tok_load.start()
    loads = load_weights((gate_hbm, up_hbm, down_hbm), (gate_w, up_w, down_w), w_sem)

    def own_copy(w):
        return remote(own_send.at[w], own_recv.at[w], own_sem.at[0, w], own_sem.at[1, w], place(0, w))

    def own_return(w):
        return remote(own_result.at[w], own_back.at[w], own_sem.at[2, w], own_sem.at[3, w], place(0, w))

    def z_part(k):
        return pl.ds(k * BASE, BASE) if k < 2 else pl.ds(2 * BASE, slot_count)

    def z_copy(w, k):
        return remote(z_send.at[w, z_part(k)], z_recv.at[w, z_part(k)], z_sem.at[0, 3 * w + k], z_sem.at[1, 3 * w + k],
                      place((2, 3, 1)[k], w))

    def z_return(w, k):
        return remote(z_result.at[w, z_part(k)], z_back.at[w, z_part(k)], z_sem.at[2, 3 * w + k], z_sem.at[3, 3 * w + k],
                      place((2, 3, 1)[k], w))

    sent = pl.ds(0, SPILL)
    kind = 1 - ((node + 1) // 2 + 1) % 2

    def list_copy(src, codes_src, at, go, device):
        w, i = at
        come = 2 * w + i
        named = pl.ds(0, 2)
        return Both(remote(src.at[sent], lists.at[w, i, sent], list_sem.at[go], list_sem.at[come], device),
                    remote(codes_src.at[named], codes_in.at[w, i, named], code_sem.at[go], code_sem.at[come], device))

    def list_out(h):
        return list_copy(list_send.at[h], codes_out.at[h], (2 * h, kind), 8 + h,
                         {"node": 2 - node // 2, "expert": flip(expert, 2 * h)})

    def arrived(w, i):
        return list_copy(lists.at[w, i], codes_in.at[w, i], (w, i), 8, place(0, 1))

    def forward_z(w, i):
        return list_copy(lists.at[w, i], codes_in.at[w, i], (w, 1 - i), 10 + w + i, place(1, 0))

    def forward_core(w, i):
        return list_copy(lists.at[w, i], codes_in.at[w, i], (w + 1, i), 14 + w + i, place(0, 1))

    def share_core(w, i):
        return remote(shares.at[w, i, sent], core_in.at[w // 2, i, sent], share_sem.at[2 * w + i],
                      share_sem.at[8 + 2 * (w // 2) + i], place(0, 1))

    def share_z(w, i):
        return remote(shares.at[w, i, sent], z_in.at[w // 2, 1 - i, sent], share_sem.at[2 * w + i],
                      share_sem.at[13 + w - i], place(1, 0))

    def share_home(w, i):
        return remote(shares.at[w, i, sent], list_back.at[w // 2, sent], share_sem.at[2 * w + i],
                      share_sem.at[16 + w // 2], place(2 + i, w))

    def flag_copy(q):
        return remote(flag_src.at[pl.ds(0, 1)], flags.at[q, pl.ds(0, 1)], flag_sem.at[0, q], flag_sem.at[1, q], place(q // 4, q % 4))

    def group_copy():
        return remote(group_src.at[pl.ds(0, 1)], group_in.at[pl.ds(0, 1)], flag_sem.at[0, 0], flag_sem.at[1, 0], twin)

    ids, slots = ids_ref[...], slots_ref[...]
    flat_pos = jnp.where(slots >= 0, ids * slot_count + slots, 16 * slot_count)
    far_spill = jnp.logical_and(ids // 8 != node // 2, slots >= BASE)
    lanes = 128
    folds = rows // lanes
    upto = one_hot(lax.broadcasted_iota(jnp.int32, (lanes, lanes), 0) <= lax.broadcasted_iota(jnp.int32, (lanes, lanes), 1))
    before = one_hot(lax.broadcasted_iota(jnp.int32, (folds, folds), 1) < lax.broadcasted_iota(jnp.int32, (folds, folds), 0))
    codes = jnp.concatenate([ids, slots] + [jnp.zeros_like(ids)] * (CODES - 2), axis=0).astype(jnp.float32).astype(jnp.bfloat16)
    excess = 0.0
    tok_load.wait()
    for h in range(2):
        column = (expert // 2 + h) % 2
        spills = jnp.logical_and(far_spill, ids // 2 % 2 == column).astype(jnp.float32)
        grid = jnp.concatenate([spills[:, i * lanes:(i + 1) * lanes] for i in range(folds)], axis=0)
        marks = grid.astype(jnp.bfloat16)
        order = matmul(marks, upto) + jnp.sum(matmul(before, marks), axis=1, keepdims=True)
        order = jnp.where(grid > 0, order, 0.0).astype(jnp.int32) - 1
        order = jnp.concatenate([order[i:i + 1, :] for i in range(folds)], axis=1)
        order = jnp.where(order < SPILL, order, -1)
        list_hot[h] = one_hot(order == lax.broadcasted_iota(jnp.int32, (PADDED, rows), 0))
        named = lax.dot_general(codes, list_hot[h], (((1,), (1,)), ((), ())), preferred_element_type=jnp.float32)
        list_send[h, 0:SPILL] = matmul(list_hot[h, 0:SPILL], tok_ref[...]).astype(jnp.bfloat16)
        codes_out[h] = named[0:8]
        list_back[h, SPILL:PADDED] = jnp.zeros((PADDED - SPILL, width), jnp.bfloat16)
        excess = jnp.maximum(excess, jnp.sum(spills) - SPILL)
    flag_src[...] = jnp.broadcast_to(excess, flag_src.shape)

    def target(by_node, w, count):
        return lax.broadcasted_iota(jnp.int32, (count, rows), 0) + expert_of(by_node, w) * slot_count

    def own_pick(w, carry):
        own_hot[w] = one_hot(flat_pos == target(0, w, slot_count))
        own_send[w] = matmul(own_hot[w], tok_ref[...]).astype(jnp.bfloat16)

        return carry

    pl.semaphore_wait(barrier, 16)
    list_out(0).start()
    list_out(1).start()

    def flag_out(q, carry):
        flag_copy(q).start()
        return carry

    lax.fori_loop(1, 16, flag_out, 0)

    def z_pick(w, carry):
        z_hot[w, 0:BASE] = one_hot(flat_pos == target(2, w, BASE))
        z_hot[w, BASE:2 * BASE] = one_hot(flat_pos == target(3, w, BASE))
        z_hot[w, 2 * BASE:] = one_hot(flat_pos == target(1, w, slot_count))
        z_send[w] = matmul(z_hot[w], tok_ref[...]).astype(jnp.bfloat16)

        for role, is_role in roles:
            early = [v for v in range(4) if role["near"][v] == 0]
            if early == [0, 1, 2, 3]:
                @pl.when(is_role)
                def _():
                    z_copy(w, 2).start()

        return carry

    lax.fori_loop(0, 4, z_pick, 0)
    lax.fori_loop(0, 4, own_pick, 0)
    for w in range(1, 4):
        own_copy(w).start()
    for w in range(4):
        for i in range(2):
            lists[w, i, SPILL:PADDED] = jnp.zeros((PADDED - SPILL, width), jnp.bfloat16)
    for load in loads:
        load.wait()

    def ffn(block):
        return expert_ffn(block, gate_w, up_w, down_w, hidden)

    own_recv[0] = own_send[0]

    def own_step(w, carry):
        @pl.when(w > 0)
        def _():
            own_copy(w).wait_recv()

        own_result[w] = ffn(own_recv[w])

        @pl.when(w > 0)
        def _():
            own_return(w).start()

        return carry


    me = node * 4 + expert
    over = slot_count - BASE

    near = slice(2 * BASE, 2 * BASE + slot_count)
    far = slice(0, 2 * BASE)

    def near_step(w, carry):
        z_copy(w, 2).wait_recv()
        z_result[w, near] = ffn(z_recv[w, near])
        return carry

    def far_step(w, carry):
        z_copy(w, 0).wait_recv()
        z_copy(w, 1).wait_recv()
        z_result[w, far] = ffn(z_recv[w, far])
        z_return(w, 0).start()
        z_return(w, 1).start()
        return carry

    def list_step(r, carry):
        i = 1 - kind + (r // 2) * (2 * kind - 1)
        odd = 1 - r % 2

        @pl.when(odd == 1)
        def _():
            @pl.when(jnp.logical_not(inner))
            def _():
                for w in (0, 2):
                    arrived(w, i).wait_recv()
                    forward_core(w, i).start()

            for w in (1, 3):
                arrived(w, i).wait_recv()

        mine, blocks = [], []
        for h in range(2):
            w = 2 * h + odd
            codes = codes_in[w, i]
            slot = lax.broadcasted_iota(jnp.int32, (over, PADDED), 0) + BASE
            hit = jnp.logical_and(codes[0:1].astype(jnp.int32) == me, codes[1:2].astype(jnp.int32) == slot)
            mine.append(one_hot(hit))
            blocks.append(matmul(mine[h], lists[w, i]).astype(jnp.bfloat16))
        y = ffn(jnp.concatenate(blocks, axis=0))
        for h in range(2):
            shares[2 * h + odd, i] = matmul_t(mine[h], y[h * over:(h + 1) * over]).astype(jnp.bfloat16)

        @pl.when(odd == 1)
        def _():
            for w in (1, 3):
                share_core(w, i).start()

        @pl.when(odd == 0)
        def _():
            for w in (0, 2):
                share_core(w + 1, i).wait_recv()
                shares[w, i, 0:SPILL] += core_in[w // 2, i, 0:SPILL]

                @pl.when(jnp.logical_not(inner))
                def _():
                    share_z(w, i).start()

        return carry

    def forward_list(w, i):
        arrived(w, i).wait_recv()
        forward_core(w, i).start()
        forward_z(w, i).start()

    def merge_home(i):
        for w in (0, 2):
            share_z(w, 1 - i).wait_recv()
            shares[w, i, 0:SPILL] += z_in[w // 2, i, 0:SPILL]
            share_home(w, i).start()

    def acts(role, slot):
        same = kind_of_far[role is INNER]
        found = []
        for w in range(4):
            if role["near"][w] == slot and role["near"] != (0, 0, 0, 0):
                found.append(z_copy(w, 2).start)
        for name, k in (("to_inner", same), ("to_outer", 1 - same)):
            found += [z_copy(w, k).start for w in range(4) if role[name][w] == slot]
        found += [z_return(w, 2).start for w in range(4) if role["near_back"][w] == slot]
        if role is INNER:
            found += [functools.partial(forward_list, w, i) for w, i, when in role["lists"] if when == slot]
            found += [functools.partial(merge_home, i) for i in (0, 1) if role["home"][i] == slot]
        return found

    kind_of_far = {True: 1, False: 0}

    def fire(at):
        for role, is_role in roles:
            for slot in range(len(role["order"])):
                todo = acts(role, slot)
                if todo:
                    @pl.when(jnp.logical_and(at == slot, is_role))
                    def _():
                        for act in todo:
                            act()

    def table(values, at):
        inner_values, outer_values = values
        total = 0
        for slot, (a, b) in enumerate(zip(inner_values, outer_values)):
            total = total + jnp.where(at == slot, a if a == b else jnp.where(inner, a, b), 0)
        return total

    orders = [role["order"] for role, _ in roles]
    sorts = [[KINDS.index(letter) for letter in order] for order in orders]
    turns = [[order[:slot].count(letter) for slot, letter in enumerate(order)] for order in orders]

    def slot_step(at, carry):
        fire(at)
        sort, turn = table(sorts, at), table(turns, at)
        for number, step in enumerate((own_step, near_step, far_step, list_step)):
            @pl.when(sort == number)
            def _():
                step(turn, 0)

        return carry

    lax.fori_loop(0, 16, slot_step, 0)
    own_back[0] = own_result[0]
    for role, is_role in roles:
        todo = acts(role, 16)
        if todo:
            @pl.when(is_role)
            def _():
                for act in todo:
                    act()

    def flag_in(q, carry):
        flag_copy(q).wait_recv()
        return carry

    lax.fori_loop(1, 16, flag_in, 0)
    flags[0] = flag_src[...]
    group_src[0:1] = jnp.max(flags[:, 0:1], axis=0)

    flag_copy(1).wait_send()
    group_copy().start()

    for w in range(1, 4):
        own_return(w).wait_recv()
    total[...] = matmul_t(own_hot[...].reshape(4 * slot_count, rows), own_back[...].reshape(4 * slot_count, width))

    def z_combine(w, carry):
        for k in (2, 0, 1):
            z_return(w, k).wait_recv()
        total[...] += matmul_t(z_hot[w], z_back[w])
        return carry

    lax.fori_loop(0, 4, z_combine, 0)
    group_copy().wait_recv()
    full_ref[0, 0] = (jnp.max(jnp.maximum(group_src[0:1], group_in[0:1])) > 0.0).astype(jnp.int32)

    for w in range(1, 4):
        own_copy(w).wait_send()
        own_return(w).wait_send()
    for w in range(4):
        for k in range(3):
            z_copy(w, k).wait_send()
            z_return(w, k).wait_send()
    group_copy().wait_send()

    def flag_sent(q, carry):
        flag_copy(q).wait_send()
        return carry

    lax.fori_loop(2, 16, flag_sent, 0)
    for i in range(2):
        list_out(i).wait_send()
        for w in (0, 2):
            forward_core(w, i).wait_send()
            share_core(w + 1, i).wait_send()

            @pl.when(inner)
            def _():
                forward_z(w, i).wait_send()
                share_home(w, i).wait_send()

            @pl.when(jnp.logical_not(inner))
            def _():
                share_z(w, i).wait_send()

    share_home(0, 0).wait_recv()
    total[...] += matmul_t(list_hot[0], list_back[0])
    share_home(2, 0).wait_recv()
    out_ref[...] = (total[...] + matmul_t(list_hot[1], list_back[1])).astype(out_ref.dtype)


def solution(mesh):
    group_size = mesh.shape["node"] * mesh.shape["expert"]
    tok_spec = P(("data", "node", "expert"), None)
    weight_spec = P(("node", "expert"), None, None)

    def local_layer(tokens, expert_ids, gate_weights, slot_ids, w_gate, w_up, w_down):
        rows, width = tokens.shape
        ff = w_gate.shape[2]
        slot_count = capacity(rows, 1, group_size)
        vmem = pl.BlockSpec(memory_space=pltpu.VMEM)
        smem = pl.BlockSpec(memory_space=pltpu.SMEM)
        hbm = pl.BlockSpec(memory_space=pl.ANY)
        dma = pltpu.SemaphoreType.DMA
        weights = [pltpu.VMEM((width, ff), jnp.bfloat16), pltpu.VMEM((width, ff), jnp.bfloat16),
                   pltpu.VMEM((ff, width), jnp.bfloat16)]
        hidden = pltpu.VMEM((2 * (slot_count - BASE), ff), jnp.bfloat16)
        total = pltpu.VMEM((rows, width), jnp.float32)
        picked_shape = jax.ShapeDtypeStruct((rows, width), jnp.bfloat16)
        operands = (tokens, expert_ids.reshape(1, rows), slot_ids.reshape(1, rows), w_gate, w_up, w_down)

        def bf16(*shape):
            return pltpu.VMEM(shape, jnp.bfloat16)

        def params(number):
            return pltpu.CompilerParams(collective_id=number, has_side_effects=True, vmem_limit_bytes=60 * 1024 * 1024)

        def scaled(picked):
            return (gate_weights * picked.astype(jnp.float32)).astype(jnp.bfloat16)

        def padded():
            block = (group_size, slot_count, width)
            return pl.pallas_call(
                functools.partial(padded_kernel, slot_count), out_shape=picked_shape,
                in_specs=[vmem] * 3 + [hbm] * 3, out_specs=vmem,
                scratch_shapes=weights + [bf16(*block)] * 4 + [hidden, total, dma((3,))] + [dma((group_size,))] * 4,
                compiler_params=params(1), name="padded_layer",
            )(*operands)

        own = (4, slot_count, width)
        zed = (4, 2 * BASE + slot_count, width)
        flag = pltpu.VMEM((8, 128), jnp.float32)
        picked, full = pl.pallas_call(
            functools.partial(packed_kernel, slot_count),
            out_shape=(picked_shape, jax.ShapeDtypeStruct((1, 1), jnp.int32)),
            in_specs=[hbm] + [vmem] * 2 + [hbm] * 3, out_specs=(vmem, smem),
            scratch_shapes=[bf16(rows, width)] + weights + [hidden, total]
            + [bf16(4, slot_count, rows)] + [bf16(*own)] * 4
            + [bf16(4, 2 * BASE + slot_count, rows)] + [bf16(*zed)] * 4
            + [bf16(2, PADDED, rows), bf16(2, PADDED, width), bf16(4, 2, PADDED, width),
               pltpu.VMEM((2, 8, PADDED), jnp.float32), pltpu.VMEM((4, 2, 8, PADDED), jnp.float32), bf16(4, 2, PADDED, width),
               bf16(2, 2, PADDED, width), bf16(2, 2, PADDED, width), bf16(2, PADDED, width)]
            + [flag, pltpu.VMEM((16, 8, 128), jnp.float32), flag, flag]
            + [dma((4,)), dma((4, 4)), dma((4, 12)), dma((18,)), dma((18,)), dma((18,)), dma((2, 16))],
            compiler_params=params(0), name="packed_layer",
        )(*operands)
        return lax.cond(full[0, 0] > 0, lambda: scaled(padded()), lambda: scaled(picked))

    return jax.shard_map(local_layer, mesh=mesh, in_specs=(tok_spec,) * 4 + (weight_spec,) * 3,
                         out_specs=tok_spec, check_vma=False)
```
